32 devices in a mesh: dp: 1 (over z), pp: 4 (over y), sp: 8 (over x, core).
Axes of the slice: x: 4, y: 4, z: 1, core: 2. Of those that a mesh axis runs over, the one named last changes fastest.
The devices are a block of a 4x4x8 slice.
Arguments:
- latent_in: float32 [4, 256, 16], P('dp', 'sp')
- pos_embed: bfloat16 [4, 256, 1152], P(None, 'sp')
- condition: bfloat16 [2, 1152], P('dp')
- step_size: float32 [2], P('dp')
- w_in: bfloat16 [16, 1152], replicated
- w_ada: bfloat16 [4, 1152, 6912], replicated
- w_qkv: bfloat16 [4, 1152, 3456], replicated
- w_o: bfloat16 [4, 1152, 1152], replicated
- w_up: bfloat16 [4, 1152, 4608], replicated
- w_down: bfloat16 [4, 4608, 1152], replicated
- b_layer: bfloat16 [4, 17280], replicated
- w_fa: bfloat16 [1152, 2304], replicated
- b_fa: bfloat16 [2304], replicated
- w_out: bfloat16 [1152, 16], replicated
- k_old: bfloat16 [4, 1024, 16, 72], P('dp')
- v_old: bfloat16 [4, 1024, 16, 72], P('dp')
Outputs:
- output: float32 [4, 256, 16], P('dp', 'sp')
All inputs are finite; a program needn't handle non-finite values.
Results may differ from the reference program's by a relative error of at most 0.0118966.
Values are sent between devices in bfloat16 or wider.
A program may use at most 768 MiB of HBM per device.

```python
import jax
import jax.numpy as jnp
from jax import lax
import math

TOKENS = 1024
PATCHES = 4
WIDTH = 1152
HEADS = 16
PATCH_DIM = 16
LAYERS = 4

PATCH_ROWS = TOKENS // PATCHES
HEAD_DIM = WIDTH // HEADS
LN_EPS = 1e-6


def setup_inputs(seed: int = 0, part: int = 0) -> dict:
    own_keys = jax.random.split(jax.random.fold_in(jax.random.key(seed), part), 7)
    shared_keys = jax.random.split(jax.random.key(seed + 1), 11)
    width_scale = WIDTH ** -0.5
    qk_boost = (math.log(TOKENS / 6.0) / 2.9) ** 0.25
    column_gain = jnp.concatenate([jnp.full((2 * WIDTH,), qk_boost, jnp.float32), jnp.ones((WIDTH,), jnp.float32)])
    buf_shape = (LAYERS, TOKENS, HEADS, HEAD_DIM)
    mean_shape = (LAYERS, 1, HEADS, HEAD_DIM)
    latent_in = jax.random.normal(own_keys[0], (PATCHES, PATCH_ROWS, PATCH_DIM), jnp.float32)
    condition = jax.random.normal(own_keys[1], (2, WIDTH), jnp.float32).astype(jnp.bfloat16)
    step_size = jax.random.uniform(own_keys[2], (2,), jnp.float32, 0.6, 1.2)
    key_mean = 0.7 * jax.random.normal(own_keys[3], mean_shape, jnp.float32)
    k_old = (1.2 * qk_boost * jax.random.normal(own_keys[4], buf_shape, jnp.float32) + key_mean).astype(jnp.bfloat16)
    value_mean = jax.random.normal(own_keys[5], mean_shape, jnp.float32)
    v_old = (jax.random.normal(own_keys[6], buf_shape, jnp.float32) + value_mean).astype(jnp.bfloat16)
    pos_embed = (0.7 * jax.random.normal(shared_keys[0], (PATCHES, PATCH_ROWS, WIDTH), jnp.float32)).astype(jnp.bfloat16)
    w_in = (jax.random.normal(shared_keys[1], (PATCH_DIM, WIDTH), jnp.float32) * PATCH_DIM ** -0.5).astype(jnp.bfloat16)
    w_ada = (jax.random.normal(shared_keys[2], (LAYERS, WIDTH, 6 * WIDTH), jnp.float32) * width_scale).astype(jnp.bfloat16)
    w_qkv = (jax.random.normal(shared_keys[3], (LAYERS, WIDTH, 3 * WIDTH), jnp.float32) * width_scale * column_gain).astype(jnp.bfloat16)
    w_o = (jax.random.normal(shared_keys[4], (LAYERS, WIDTH, WIDTH), jnp.float32) * width_scale).astype(jnp.bfloat16)
    w_up = (jax.random.normal(shared_keys[5], (LAYERS, WIDTH, 4 * WIDTH), jnp.float32) * width_scale).astype(jnp.bfloat16)
    w_down = (jax.random.normal(shared_keys[6], (LAYERS, 4 * WIDTH, WIDTH), jnp.float32) * (4 * WIDTH) ** -0.5).astype(jnp.bfloat16)
    b_layer = (0.3 * jax.random.normal(shared_keys[7], (LAYERS, 15 * WIDTH), jnp.float32)).astype(jnp.bfloat16)
    w_fa = (jax.random.normal(shared_keys[8], (WIDTH, 2 * WIDTH), jnp.float32) * width_scale).astype(jnp.bfloat16)
    b_fa = (0.3 * jax.random.normal(shared_keys[9], (2 * WIDTH,), jnp.float32)).astype(jnp.bfloat16)
    w_out = (jax.random.normal(shared_keys[10], (WIDTH, PATCH_DIM), jnp.float32) * width_scale).astype(jnp.bfloat16)
    return {"latent_in": latent_in, "pos_embed": pos_embed, "condition": condition, "step_size": step_size, "w_in": w_in, "w_ada": w_ada, "w_qkv": w_qkv, "w_o": w_o, "w_up": w_up, "w_down": w_down, "b_layer": b_layer, "w_fa": w_fa, "b_fa": b_fa, "w_out": w_out, "k_old": k_old, "v_old": v_old}


def layer_norm(hidden):
    mean_val = jnp.mean(hidden, axis=-1, keepdims=True)
    centered = hidden - mean_val
    var_val = jnp.mean(centered * centered, axis=-1, keepdims=True)
    return centered * lax.rsqrt(var_val + LN_EPS)


def attend_head(operands):
    query_head, key_head, value_head = operands
    logits = jnp.dot(query_head, key_head.T, preferred_element_type=jnp.float32) * HEAD_DIM ** -0.5
    attn_prob = jax.nn.softmax(logits, axis=-1).astype(jnp.bfloat16)
    return jnp.dot(attn_prob, value_head, preferred_element_type=jnp.float32).astype(jnp.bfloat16)


def reference(latent_in, pos_embed, condition, step_size, w_in, w_ada, w_qkv, w_o, w_up, w_down, b_layer, w_fa, b_fa, w_out, k_old, v_old):
    bias_f32 = b_layer.astype(jnp.float32)
    key_bufs = k_old
    value_bufs = v_old
    latent = latent_in
    for step_idx in range(2):
        cond_act = jax.nn.silu(condition[step_idx].astype(jnp.float32)).astype(jnp.bfloat16)
        mod_all = jnp.einsum("c,lcf->lf", cond_act.astype(jnp.float32), w_ada.astype(jnp.float32)) + bias_f32[:, :6 * WIDTH]
        final_mod = jnp.dot(cond_act[None, :], w_fa, preferred_element_type=jnp.float32)[0] + b_fa.astype(jnp.float32)
        scale_out, shift_out = jnp.split(final_mod, 2)
        step_val = step_size[step_idx]
        latent_now = latent

        def patch_body(buffers, patch_idx):
            key_all, value_all = buffers
            row_start = patch_idx * PATCH_ROWS
            x_patch = latent_now[patch_idx]

            def block(hidden, layer_in):
                mod_vec, qkv_weight, out_weight, up_weight, down_weight, bias_row, key_buf, value_buf = layer_in
                scale_attn, shift_attn, gate_attn, scale_mlp, shift_mlp, gate_mlp = jnp.split(mod_vec, 6)
                normed = (layer_norm(hidden.astype(jnp.float32)) * (1.0 + scale_attn) + shift_attn).astype(jnp.bfloat16)
                qkv_rows = (jnp.dot(normed, qkv_weight, preferred_element_type=jnp.float32) + bias_row[6 * WIDTH:9 * WIDTH]).astype(jnp.bfloat16)
                query_rows = qkv_rows[:, :WIDTH].reshape(PATCH_ROWS, HEADS, HEAD_DIM)
                key_buf = lax.dynamic_update_slice_in_dim(key_buf, qkv_rows[:, WIDTH:2 * WIDTH].reshape(PATCH_ROWS, HEADS, HEAD_DIM), row_start, axis=0)
                value_buf = lax.dynamic_update_slice_in_dim(value_buf, qkv_rows[:, 2 * WIDTH:].reshape(PATCH_ROWS, HEADS, HEAD_DIM), row_start, axis=0)
                attn_heads = lax.map(attend_head, (jnp.transpose(query_rows, (1, 0, 2)), jnp.transpose(key_buf, (1, 0, 2)), jnp.transpose(value_buf, (1, 0, 2))))
                attn_rows = jnp.transpose(attn_heads, (1, 0, 2)).reshape(PATCH_ROWS, WIDTH)
                residual = hidden.astype(jnp.float32) + gate_attn * (jnp.dot(attn_rows, out_weight, preferred_element_type=jnp.float32) + bias_row[9 * WIDTH:10 * WIDTH])
                mlp_in = (layer_norm(residual) * (1.0 + scale_mlp) + shift_mlp).astype(jnp.bfloat16)
                mlp_mid = jax.nn.gelu(jnp.dot(mlp_in, up_weight, preferred_element_type=jnp.float32) + bias_row[10 * WIDTH:14 * WIDTH], approximate=True).astype(jnp.bfloat16)
                hidden = (residual + gate_mlp * (jnp.dot(mlp_mid, down_weight, preferred_element_type=jnp.float32) + bias_row[14 * WIDTH:])).astype(jnp.bfloat16)
                return hidden, (key_buf, value_buf)

            hidden = (jnp.dot(x_patch.astype(jnp.bfloat16), w_in, preferred_element_type=jnp.float32) + pos_embed[patch_idx].astype(jnp.float32)).astype(jnp.bfloat16)
            hidden, (key_all, value_all) = lax.scan(block, hidden, (mod_all, w_qkv, w_o, w_up, w_down, bias_f32, key_all, value_all))
            out_in = (layer_norm(hidden.astype(jnp.float32)) * (1.0 + scale_out) + shift_out).astype(jnp.bfloat16)
            velocity = jnp.dot(out_in, w_out, preferred_element_type=jnp.float32)
            return (key_all, value_all), x_patch + step_val * velocity

        (key_bufs, value_bufs), latent = lax.scan(patch_body, (key_bufs, value_bufs), jnp.arange(PATCHES))
    return latent
```

```python
import functools

import jax
import jax.numpy as jnp
from jax import lax
from jax.experimental import pallas as pl
from jax.experimental.pallas import tpu as pltpu
from jax.sharding import PartitionSpec as P

LN_EPS = 1e-6
LANES = 128
LOG2_E = 1.4426950408889634
MESH = pl.DeviceIdType.MESH


def normalize(hidden):
    mean_val = jnp.mean(hidden, axis=-1, keepdims=True)
    centered = hidden - mean_val
    var_val = jnp.mean(centered * centered, axis=-1, keepdims=True)
    return centered * lax.rsqrt(var_val + LN_EPS)


def kernel(dims, latent_ref, pos_ref, cond_ref, step_ref, w_in_ref, b_layer_ref, b_fa_ref, w_out_ref,
           old_hbm, w_ada_hbm, w_fa_hbm, w_qkv_hbm, w_o_hbm, w_up_hbm, w_down_hbm,
           out_ref,
           ada_w, fa_w, qkv_w, o_w, up_w, down_w, kv, qkv_s, msg, o_msg, o_in, ada_msg, ada_in,
           mod_s, fmod_s, bias_s, hid_s, lat_s, pos_s, mid_s, lat_in, pos_in, out_in,
           w_sem, load_sem, ada_ss, ada_rs, qkv_ss, qkv_rs, o_ss, o_rs, fwd_ss, fwd_rs, in_ss, in_rs, out_ss, out_rs):
    (chips_x, chips_y, layers, patches, block_rows, width, heads, head_dim) = dims
    chips = chips_x * chips_y
    group = chips_y // 2
    patch_rows = block_rows * 2 * chips_x
    half_rows = 2 * patch_rows
    dp = lax.axis_index("dp")
    y = lax.axis_index("pp")
    s = lax.axis_index("sp")
    x = s // 2
    c = s % 2
    g = y * chips_x + x
    j_own = y // group
    patch = 2 * c + j_own
    row_own = pl.multiple_of(patch * patch_rows + (2 * x + y % 2) * block_rows, block_rows)

    def chip_dev(chip, core):
        return (dp, chip // chips_x, 2 * (chip % chips_x) + core)

    def local_row(chip):
        cy = chip // chips_x
        cx = chip % chips_x
        return (cy // group) * patch_rows + (2 * cx + cy % 2) * block_rows

    def half_row(chip):
        return pl.multiple_of(c * half_rows + local_row(chip), block_rows)

    partner = (dp, y, 2 * x + (1 - c))

    ada_tiles = ada_w.shape[1] // LANES
    ada_total = w_ada_hbm.shape[2] // LANES
    parts = chips // layers
    fa_tiles = fa_w.shape[1] // LANES
    fa_total = w_fa_hbm.shape[1] // LANES

    ada_layer = g // parts
    ada_col = pl.multiple_of(jnp.minimum(ada_tiles * (g % parts), ada_total - ada_tiles) * LANES, LANES)
    fa_col = pl.multiple_of(jnp.minimum(fa_tiles * g, fa_total - fa_tiles) * LANES, LANES)
    ada_copy = pltpu.make_async_copy(w_ada_hbm.at[ada_layer, :, pl.ds(ada_col, ada_w.shape[1])], ada_w, load_sem.at[0])
    ada_copy.start()
    fa_copy = pltpu.make_async_copy(w_fa_hbm.at[:, pl.ds(fa_col, fa_w.shape[1])], fa_w, load_sem.at[1])
    fa_copy.start()

    def w_copy(which, layer):
        src, dst = ((w_qkv_hbm, qkv_w), (w_o_hbm, o_w), (w_up_hbm, up_w), (w_down_hbm, down_w))[which]
        return pltpu.make_async_copy(src.at[layer], dst, w_sem.at[which])

    w_copy(0, 0).start()
    old_copy = pltpu.make_async_copy(old_hbm, kv.at[0], load_sem.at[2])
    old_copy.start()
    for which in range(1, 4):
        w_copy(which, 0).start()

    barrier = pltpu.get_barrier_semaphore()
    for k in range(1, chips):
        pl.semaphore_signal(barrier, inc=1, device_id=chip_dev((g + k) % chips, c), device_id_type=MESH)
    for k in range(chips_y):
        pl.semaphore_signal(barrier, inc=1, device_id=(dp, (y + k) % chips_y, 2 * x + (1 - c)), device_id_type=MESH)
    pl.semaphore_wait(barrier, chips - 1 + chips_y)

    aligned = c == y % 2
    give = 2 * (1 - c) + j_own

    def give_copies():
        return (pltpu.make_async_remote_copy(latent_ref.at[give], lat_in, in_ss.at[0], in_rs.at[0], device_id=partner, device_id_type=MESH),
                pltpu.make_async_remote_copy(pos_ref.at[give], pos_in, in_ss.at[1], in_rs.at[1], device_id=partner, device_id_type=MESH))

    @pl.when(aligned)
    def _():
        for copy in give_copies():
            copy.start()
        lat_s[...] = latent_ref[patch]
        pos_s[...] = pos_ref[patch]

    cond = cond_ref[...].astype(jnp.float32)
    act = (cond * jax.nn.sigmoid(cond)).astype(jnp.bfloat16)
    ada_copy.wait()
    ada_res = jnp.dot(act, ada_w[...], preferred_element_type=jnp.float32)
    fa_copy.wait()
    fa_res = jnp.dot(act, fa_w[...], preferred_element_type=jnp.float32)
    for t in range(2):
        for i in range(ada_tiles):
            ada_msg[t * ada_tiles + i:t * ada_tiles + i + 1, :] = ada_res[t:t + 1, i * LANES:(i + 1) * LANES]
        for i in range(fa_tiles):
            row = 2 * ada_tiles + t * fa_tiles + i
            ada_msg[row:row + 1, :] = fa_res[t:t + 1, i * LANES:(i + 1) * LANES]

    def ada_send(k):
        dest = (g + k) % chips
        return pltpu.make_async_remote_copy(ada_msg, ada_in.at[g], ada_ss.at[dest], ada_rs.at[g], device_id=chip_dev(dest, c), device_id_type=MESH)

    def ada_recv(k):
        src = (g + k) % chips
        return pltpu.make_async_remote_copy(ada_msg, ada_in.at[src], ada_ss.at[src], ada_rs.at[src], device_id=chip_dev(src, c), device_id_type=MESH)

    for k in range(1, chips):
        ada_send(k).start()
    ada_in[g] = ada_msg[...]
    bias_s[...] = b_layer_ref[...].astype(jnp.float32)

    @pl.when(aligned)
    def _():
        for copy in give_copies():
            copy.wait_send()

    @pl.when(jnp.logical_not(aligned))
    def _():
        for copy in give_copies():
            copy.wait_recv()
        lat_s[...] = lat_in[...]
        pos_s[...] = pos_in[...]

    for k in range(1, chips):
        ada_recv(k).wait_recv()
    for t in range(2):
        for layer in range(layers):
            for tile in range(ada_total):
                part = min(tile // ada_tiles, parts - 1)
                first = min(ada_tiles * part, ada_total - ada_tiles)
                row = t * ada_tiles + tile - first
                cols = slice(tile * LANES, (tile + 1) * LANES)
                mod_s[t * layers + layer:t * layers + layer + 1, cols] = ada_in[layer * parts + part, row:row + 1, :] + bias_s[layer:layer + 1, cols]
        for tile in range(fa_total):
            row = 2 * ada_tiles + t * fa_tiles + tile % fa_tiles
            cols = slice(tile * LANES, (tile + 1) * LANES)
            fmod_s[t:t + 1, cols] = ada_in[tile // fa_tiles, row:row + 1, :] + b_fa_ref[0:1, cols].astype(jnp.float32)
    for k in range(1, chips):
        ada_send(k).wait_send()
    old_copy.wait()

    lane2 = lax.broadcasted_iota(jnp.int32, (1, 2 * LANES), 1)
    lane1 = lax.broadcasted_iota(jnp.int32, (1, LANES), 1)
    factor = LOG2_E * head_dim ** -0.5
    tiles = width // LANES
    all_tiles = 3 * tiles

    def window(col, place):
        tile = min(col // LANES, all_tiles - 2)
        shift = (place - (col - tile * LANES)) % (2 * LANES)
        part = qkv_s[:, tile * LANES:(tile + 2) * LANES]
        return pltpu.roll(part, shift, 1) if shift else part

    def layer_pass(it, carry):
        t = it // layers
        layer = it % layers
        following = (it + 1) % layers
        more = it + 1 < 2 * layers
        fresh = 1 - t
        bias = lambda lo, hi: bias_s[pl.ds(layer, 1), lo * width:hi * width]
        mod = lambda i: mod_s[pl.ds(it, 1), i * width:(i + 1) * width]

        @pl.when(layer == 0)
        def _():
            emb = jnp.dot(lat_s[...].astype(jnp.bfloat16), w_in_ref[...], preferred_element_type=jnp.float32)
            hid_s[...] = (emb + pos_s[...].astype(jnp.float32)).astype(jnp.bfloat16)

        normed = (normalize(hid_s[...].astype(jnp.float32)) * (1.0 + mod(0)) + mod(1)).astype(jnp.bfloat16)
        w_copy(0, layer).wait()
        for i in (1, 2, 0):
            cols = slice(i * width, (i + 1) * width)
            part = jnp.dot(normed, qkv_w[:, cols], preferred_element_type=jnp.float32) + bias(6 + i, 7 + i)
            qkv_s[:, cols] = part.astype(jnp.bfloat16).astype(jnp.float32)

        @pl.when(more)
        def _():
            w_copy(0, following).start()

        for head in range(heads):
            at = head * head_dim
            block = jnp.where(lane2 < head_dim, window(width + at, 0),
                              jnp.where(lane2 < 2 * head_dim, window(2 * width + at, head_dim), window(at, 2 * head_dim)))
            msg[head] = block.astype(jnp.bfloat16)

        def qkv_send(k):
            dest = (g + k) % chips
            return pltpu.make_async_remote_copy(msg.at[dest], kv.at[fresh, layer, pl.ds(row_own, block_rows), :], qkv_ss.at[dest], qkv_rs.at[g], device_id=chip_dev(dest, c), device_id_type=MESH)

        def qkv_recv(k):
            src = (g + k) % chips
            return pltpu.make_async_remote_copy(msg.at[src], kv.at[fresh, layer, pl.ds(half_row(src), block_rows), :], qkv_ss.at[src], qkv_rs.at[src], device_id=chip_dev(src, c), device_id_type=MESH)

        for k in range(1, chips):
            qkv_send(k).start()
        kv[fresh, layer, pl.ds(row_own, block_rows), :] = msg[g]
        for k in range(1, chips):
            qkv_recv(k).wait_recv()

        def forward():
            rows = pl.ds(pl.multiple_of(c * half_rows, half_rows), half_rows)
            return pltpu.make_async_remote_copy(kv.at[fresh, layer, rows, :], kv.at[fresh, layer, rows, :], fwd_ss.at[layer], fwd_rs.at[layer], device_id=partner, device_id_type=MESH)

        def forwarded(slot):
            rows = pl.ds(pl.multiple_of((1 - c) * half_rows, half_rows), half_rows)
            return pltpu.make_async_remote_copy(kv.at[slot, layer, rows, :], kv.at[slot, layer, rows, :], fwd_ss.at[layer], fwd_rs.at[layer], device_id=partner, device_id_type=MESH)

        @pl.when(jnp.logical_and(c == 0, t == 1))
        def _():
            forwarded(1).wait_recv()

        @pl.when(c == 0)
        def _():
            forward().start()

        @pl.when(c == 1)
        def _():
            forwarded(fresh).wait_recv()

        for j in range(2):
            p = 2 * c + j
            q_rows = pl.ds(pl.multiple_of(p * patch_rows, patch_rows), patch_rows)
            q_part = pltpu.roll(kv[fresh, layer, q_rows, LANES:].astype(jnp.float32), 2 * LANES - 2 * head_dim, 1)
            q_part = jnp.where(lane1 < head_dim, q_part, 0.0).astype(jnp.bfloat16)
            slots = [jnp.where(kp <= p, fresh, 1 - fresh) for kp in range(patches)]
            scores = jnp.concatenate(
                [lax.dot_general(q_part, kv[slots[kp], layer, kp * patch_rows:(kp + 1) * patch_rows, :LANES], (((1,), (1,)), ((), ())), preferred_element_type=jnp.float32)
                 for kp in range(patches)], axis=1)
            top = jnp.max(scores, axis=-1, keepdims=True)
            e = jnp.exp2((scores - top) * factor)
            prob = (e * (1.0 / jnp.sum(e, axis=-1, keepdims=True))).astype(jnp.bfloat16)
            o = None
            for kp in range(patches):
                term = jnp.dot(prob[:, kp * patch_rows:(kp + 1) * patch_rows], kv[slots[kp], layer, kp * patch_rows:(kp + 1) * patch_rows, :], preferred_element_type=jnp.float32)
                o = term if o is None else o + term
            o_msg[j * patch_rows:(j + 1) * patch_rows, :] = pltpu.roll(o, 2 * LANES - head_dim, 1)[:, :LANES].astype(jnp.bfloat16)

        def o_send(k):
            dest = (g + k) % chips
            rows = pl.ds(pl.multiple_of(local_row(dest), block_rows), block_rows)
            return pltpu.make_async_remote_copy(o_msg.at[rows, :], o_in.at[g], o_ss.at[dest], o_rs.at[g], device_id=chip_dev(dest, c), device_id_type=MESH)

        def o_recv(k):
            src = (g + k) % chips
            return pltpu.make_async_remote_copy(o_msg.at[pl.ds(0, block_rows), :], o_in.at[src], o_ss.at[src], o_rs.at[src], device_id=chip_dev(src, c), device_id_type=MESH)

        for k in range(1, chips):
            o_send(k).start()
        o_in[g] = o_msg[pl.ds(pl.multiple_of(local_row(g), block_rows), block_rows), :]

        @pl.when(jnp.logical_and(c == 1, t == 0))
        def _():
            forward().start()

        for k in range(1, chips):
            o_recv(k).wait_recv()

        pieces = [None] * tiles
        for head in range(heads):
            at = head * head_dim
            tile, off = at // LANES, at % LANES
            part = o_in[head].astype(jnp.float32)
            if off:
                part = pltpu.roll(part, off, 1)
            pieces[tile] = part if pieces[tile] is None else jnp.where(lane1 >= off, part, pieces[tile])
            if off + head_dim > LANES:
                pieces[tile + 1] = part
        attn = jnp.concatenate(pieces, axis=1).astype(jnp.bfloat16)
        w_copy(1, layer).wait()
        proj = jnp.dot(attn, o_w[...], preferred_element_type=jnp.float32) + bias(9, 10)

        @pl.when(more)
        def _():
            w_copy(1, following).start()

        residual = hid_s[...].astype(jnp.float32) + mod(2) * proj
        mlp_in = (normalize(residual) * (1.0 + mod(3)) + mod(4)).astype(jnp.bfloat16)
        w_copy(2, layer).wait()
        for i in range(4):
            cols = slice(i * width, (i + 1) * width)
            up = jnp.dot(mlp_in, up_w[:, cols], preferred_element_type=jnp.float32) + bias(10 + i, 11 + i)
            mid_s[:, cols] = jax.nn.gelu(up, approximate=True).astype(jnp.bfloat16)

        @pl.when(more)
        def _():
            w_copy(2, following).start()

        w_copy(3, layer).wait()
        down = jnp.dot(mid_s[...], down_w[...], preferred_element_type=jnp.float32) + bias(14, 15)
        hid_s[...] = (residual + mod(5) * down).astype(jnp.bfloat16)

        @pl.when(more)
        def _():
            w_copy(3, following).start()

        @pl.when(layer == layers - 1)
        def _():
            scale_out = fmod_s[pl.ds(t, 1), :width]
            shift_out = fmod_s[pl.ds(t, 1), width:]
            out_rows = (normalize(hid_s[...].astype(jnp.float32)) * (1.0 + scale_out) + shift_out).astype(jnp.bfloat16)
            velocity = jnp.dot(out_rows, w_out_ref[...], preferred_element_type=jnp.float32)
            lat_s[...] = lat_s[...] + step_ref[t] * velocity

        for k in range(1, chips):
            qkv_send(k).wait_send()
            o_send(k).wait_send()

        @pl.when(jnp.logical_or(c == 0, t == 0))
        def _():
            forward().wait_send()

        return carry

    lax.fori_loop(0, 2 * layers, layer_pass, 0)

    home = 2 * x + y % 2

    def out_send(cy):
        return pltpu.make_async_remote_copy(lat_s, out_in.at[patch], out_ss.at[cy], out_rs.at[patch], device_id=(dp, cy, home), device_id_type=MESH)

    def is_self(cy):
        return jnp.logical_and(cy == y, aligned)

    for k in range(chips_y):
        cy = (y + k) % chips_y

        @pl.when(jnp.logical_not(is_self(cy)))
        def _():
            out_send(cy).start()

    @pl.when(aligned)
    def _():
        out_in[patch] = lat_s[...]

    for p in range(patches):
        @pl.when(jnp.logical_not(jnp.logical_and(aligned, patch == p)))
        def _():
            pltpu.make_async_remote_copy(lat_s, out_in.at[p], out_ss.at[p], out_rs.at[p], device_id=(dp, y, home), device_id_type=MESH).wait_recv()
    out_ref[...] = out_in[...]
    for k in range(chips_y):
        cy = (y + k) % chips_y

        @pl.when(jnp.logical_not(is_self(cy)))
        def _():
            out_send(cy).wait_send()


def solution(mesh):
    chips_y = mesh.shape["pp"]
    chips_x = mesh.shape["sp"] // 2
    chips = chips_x * chips_y
    row_spec = P("dp", "sp", None)
    full_spec = P()
    buf_spec = P("dp", None, None, None)
    in_specs = (row_spec, P(None, "sp", None), P("dp", None), P("dp"), full_spec, full_spec, full_spec, full_spec, full_spec, full_spec, full_spec, full_spec, full_spec, full_spec, buf_spec, buf_spec)

    def device_fn(latent_in, pos_embed, condition, step_size, w_in, w_ada, w_qkv, w_o, w_up, w_down, b_layer, w_fa, b_fa, w_out, k_old, v_old):
        patches, block_rows, latent_dim = latent_in.shape
        layers, width = w_qkv.shape[:2]
        tokens, heads, head_dim = k_old.shape[1:]
        my_head = lax.axis_index("pp") * chips_x + lax.axis_index("sp") // 2
        k_head = lax.dynamic_index_in_dim(k_old, my_head, axis=2, keepdims=False)
        v_head = lax.dynamic_index_in_dim(v_old, my_head, axis=2, keepdims=False)
        old_kv = jnp.concatenate([k_head, v_head, jnp.zeros((layers, tokens, 2 * LANES - 2 * head_dim), k_old.dtype)], axis=-1)
        parts = chips // layers
        ada_tiles = -(-(w_ada.shape[2] // LANES) // parts)
        fa_tiles = -(-(w_fa.shape[1] // LANES) // chips)
        ada_rows = 2 * (ada_tiles + fa_tiles)
        half_rows = 2 * block_rows * 2 * chips_x
        dims = (chips_x, chips_y, layers, patches, block_rows, width, heads, head_dim)
        bf16, f32 = jnp.bfloat16, jnp.float32
        vmem = pl.BlockSpec(memory_space=pltpu.VMEM)
        hbm = pl.BlockSpec(memory_space=pl.ANY)
        dma = pltpu.SemaphoreType.DMA
        return pl.pallas_call(
            functools.partial(kernel, dims),
            out_shape=jax.ShapeDtypeStruct(latent_in.shape, f32),
            in_specs=[vmem, vmem, vmem, pl.BlockSpec(memory_space=pltpu.SMEM), vmem, vmem, vmem, vmem] + [hbm] * 7,
            out_specs=vmem,
            scratch_shapes=[
                pltpu.VMEM((width, ada_tiles * LANES), bf16),
                pltpu.VMEM((width, fa_tiles * LANES), bf16),
                pltpu.VMEM(w_qkv.shape[1:], bf16),
                pltpu.VMEM(w_o.shape[1:], bf16),
                pltpu.VMEM(w_up.shape[1:], bf16),
                pltpu.VMEM(w_down.shape[1:], bf16),
                pltpu.VMEM((2, layers, tokens, 2 * LANES), bf16),
                pltpu.VMEM((block_rows, 3 * width), f32),
                pltpu.VMEM((chips, block_rows, 2 * LANES), bf16),
                pltpu.VMEM((half_rows, LANES), bf16),
                pltpu.VMEM((chips, block_rows, LANES), bf16),
                pltpu.VMEM((ada_rows, LANES), f32),
                pltpu.VMEM((chips, ada_rows, LANES), f32),
                pltpu.VMEM((2 * layers, w_ada.shape[2]), f32),
                pltpu.VMEM((2, w_fa.shape[1]), f32),
                pltpu.VMEM(b_layer.shape, f32),
                pltpu.VMEM((block_rows, width), bf16),
                pltpu.VMEM((block_rows, latent_dim), f32),
                pltpu.VMEM((block_rows, width), bf16),
                pltpu.VMEM((block_rows, w_up.shape[2]), bf16),
                pltpu.VMEM((block_rows, latent_dim), f32),
                pltpu.VMEM((block_rows, width), bf16),
                pltpu.VMEM((patches, block_rows, latent_dim), f32),
                dma((4,)), dma((3,)), dma((chips,)), dma((chips,)), dma((chips,)), dma((chips,)), dma((chips,)), dma((chips,)),
                dma((layers,)), dma((layers,)), dma((2,)), dma((2,)), dma((chips_y,)), dma((patches,)),
            ],
            compiler_params=pltpu.CompilerParams(collective_id=0, has_side_effects=True, vmem_limit_bytes=60 * 1024 * 1024),
        )(latent_in, pos_embed, condition, step_size, w_in, b_layer, b_fa[None, :], w_out, old_kv, w_ada, w_fa, w_qkv, w_o, w_up, w_down)

    return jax.shard_map(device_fn, mesh=mesh, in_specs=in_specs, out_specs=row_spec, check_vma=False)
```

```python
import functools

import jax
import jax.numpy as jnp
from jax import lax
from jax.experimental import pallas as pl
from jax.experimental.pallas import tpu as pltpu
from jax.sharding import PartitionSpec as P

LN_EPS = 1e-6
LANES = 128
LOG2_E = 1.4426950408889634
MESH = pl.DeviceIdType.MESH


def normalize(hidden):
    mean_val = jnp.mean(hidden, axis=-1, keepdims=True)
    centered = hidden - mean_val
    var_val = jnp.mean(centered * centered, axis=-1, keepdims=True)
    return centered * lax.rsqrt(var_val + LN_EPS)


def kernel(dims, latent_ref, cond_ref, step_ref, w_in_ref, b_fa_ref, w_out_ref,
           pos_hbm, b_layer_hbm, k_hbm, v_hbm, w_ada_hbm, w_fa_hbm, w_qkv_hbm, w_o_hbm, w_up_hbm, w_down_hbm,
           out_ref,
           ada_w, fa_w, qkv_w, o_w, up_w, down_w, kv, old_s, qkv_s, msg, o_msg, o_in, ada_msg, ada_in,
           mod_s, fmod_s, bias_in, bias_s, hid_s, lat_s, pos_s, mid_s, out_in,
           w_sem, load_sem, ada_ss, ada_rs, qkv_ss, qkv_rs, o_ss, o_rs, fwd_ss, fwd_rs, out_ss, out_rs):
    (chips_x, chips_y, layers, block_rows, width, heads, head_dim) = dims
    blocks = 2 * chips_x
    patch_rows = block_rows * blocks
    half_rows = 2 * patch_rows
    members = 2 * blocks
    far_order = sorted(range(chips_x), key=lambda d: -min(d, chips_x - d))
    dp = lax.axis_index("dp")
    y = lax.axis_index("pp")
    s = lax.axis_index("sp")
    x = s // 2
    core = s % 2
    upper = y // 2
    lane_row = y % 2
    own_group = jnp.where(upper == 0, lane_row, 1 - lane_row)
    my_head = own_group * blocks + s
    row_own = pl.multiple_of(y * patch_rows + s * block_rows, block_rows)

    def group_row(group):
        return jnp.where(upper == 0, group, chips_y - 1 - group)

    def column(dx, dc):
        return 2 * ((x + dx) % chips_x) + (core + dc) % 2

    def device_row(head):
        return group_row(head // blocks)

    def dev(head):
        return (dp, device_row(head), head % blocks)

    others = [(flip, dx, dc) for flip in (1, 0) for dx in far_order for dc in (1, 0) if (flip, dx, dc) != (0, 0, 0)]

    def member(flip, dx, dc):
        return (own_group + flip) % 2 * blocks + column(dx, dc)

    partner = (dp, chips_y - 1 - y, s)

    ada_tiles = ada_w.shape[1] // LANES
    ada_total = w_ada_hbm.shape[2] // LANES
    parts = members // layers
    fa_tiles = fa_w.shape[1] // LANES
    fa_total = w_fa_hbm.shape[1] // LANES

    ada_col = pl.multiple_of(jnp.minimum(ada_tiles * (my_head % parts), ada_total - ada_tiles) * LANES, LANES)
    fa_col = pl.multiple_of(jnp.minimum(fa_tiles * my_head, fa_total - fa_tiles) * LANES, LANES)
    ada_copy = pltpu.make_async_copy(w_ada_hbm.at[my_head // parts, :, pl.ds(ada_col, ada_w.shape[1])], ada_w, load_sem.at[0])
    ada_copy.start()
    fa_copy = pltpu.make_async_copy(w_fa_hbm.at[:, pl.ds(fa_col, fa_w.shape[1])], fa_w, load_sem.at[1])
    fa_copy.start()
    bias_copy = pltpu.make_async_copy(b_layer_hbm, bias_in, load_sem.at[2])
    bias_copy.start()
    pos_copy = pltpu.make_async_copy(pos_hbm.at[y], pos_s, load_sem.at[3])
    pos_copy.start()

    def w_copy(which, layer):
        src, dst = ((w_qkv_hbm, qkv_w), (w_o_hbm, o_w), (w_up_hbm, up_w), (w_down_hbm, down_w))[which]
        return pltpu.make_async_copy(src.at[layer], dst, w_sem.at[which])

    w_copy(0, 0).start()
    k_copy = pltpu.make_async_copy(k_hbm.at[:, my_head], old_s.at[0], load_sem.at[4])
    v_copy = pltpu.make_async_copy(v_hbm.at[:, my_head], old_s.at[1], load_sem.at[5])
    k_copy.start()
    v_copy.start()
    for which in range(1, 4):
        w_copy(which, 0).start()

    barrier = pltpu.get_barrier_semaphore()
    for flip, dx, dc in others:
        pl.semaphore_signal(barrier, inc=1, device_id=dev(member(flip, dx, dc)), device_id_type=MESH)
    for k in range(2):
        pl.semaphore_signal(barrier, inc=1, device_id=(dp, (1 - upper) * 2 + k, s), device_id_type=MESH)
    pl.semaphore_wait(barrier, members + 1)

    cond = cond_ref[...].astype(jnp.float32)
    act = (cond * jax.nn.sigmoid(cond)).astype(jnp.bfloat16)
    ada_copy.wait()
    ada_res = jnp.dot(act, ada_w[...], preferred_element_type=jnp.float32)
    fa_copy.wait()
    fa_res = jnp.dot(act, fa_w[...], preferred_element_type=jnp.float32)
    for t in range(2):
        for i in range(ada_tiles):
            ada_msg[t * ada_tiles + i:t * ada_tiles + i + 1, :] = ada_res[t:t + 1, i * LANES:(i + 1) * LANES]
        for i in range(fa_tiles):
            row = 2 * ada_tiles + t * fa_tiles + i
            ada_msg[row:row + 1, :] = fa_res[t:t + 1, i * LANES:(i + 1) * LANES]

    def ada_send(other):
        dest = member(*other)
        return pltpu.make_async_remote_copy(ada_msg, ada_in.at[my_head], ada_ss.at[dest], ada_rs.at[my_head], device_id=dev(dest), device_id_type=MESH)

    def ada_recv(other):
        src = member(*other)
        return pltpu.make_async_remote_copy(ada_msg, ada_in.at[src], ada_ss.at[src], ada_rs.at[src], device_id=dev(src), device_id_type=MESH)

    for other in others:
        ada_send(other).start()
    ada_in[my_head] = ada_msg[...]
    bias_copy.wait()
    bias_s[...] = bias_in[...].astype(jnp.float32)
    lat_s[...] = latent_ref[y]
    pos_copy.wait()
    k_copy.wait()
    v_copy.wait()
    for other in others:
        ada_recv(other).wait_recv()
    for t in range(2):
        for layer in range(layers):
            for tile in range(ada_total):
                part = min(tile // ada_tiles, parts - 1)
                first = min(ada_tiles * part, ada_total - ada_tiles)
                row = t * ada_tiles + tile - first
                cols = slice(tile * LANES, (tile + 1) * LANES)
                mod_s[t * layers + layer:t * layers + layer + 1, cols] = ada_in[layer * parts + part, row:row + 1, :] + bias_s[layer:layer + 1, cols]
        for tile in range(fa_total):
            row = 2 * ada_tiles + t * fa_tiles + tile % fa_tiles
            cols = slice(tile * LANES, (tile + 1) * LANES)
            fmod_s[t:t + 1, cols] = ada_in[tile // fa_tiles, row:row + 1, :] + b_fa_ref[0:1, cols].astype(jnp.float32)
    for other in others:
        ada_send(other).wait_send()

    lane2 = lax.broadcasted_iota(jnp.int32, (1, 2 * LANES), 1)
    lane1 = lax.broadcasted_iota(jnp.int32, (1, LANES), 1)
    factor = LOG2_E * head_dim ** -0.5
    tiles = width // LANES
    group_tiles = -(-(blocks * head_dim) // LANES)

    def layer_pass(it, carry):
        t = it // layers
        layer = it % layers
        following = (it + 1) % layers
        more = it + 1 < 2 * layers
        fresh = 1 - t
        bias = lambda lo, hi: bias_s[pl.ds(layer, 1), lo * width:hi * width]
        mod = lambda i: mod_s[pl.ds(it, 1), i * width:(i + 1) * width]

        @pl.when(layer == 0)
        def _():
            emb = lax.dot_general(lat_s[...].astype(jnp.bfloat16), w_in_ref[...], (((0,), (0,)), ((), ())), preferred_element_type=jnp.float32)
            hid_s[...] = (emb + pos_s[...].astype(jnp.float32)).astype(jnp.bfloat16)

        normed = (normalize(hid_s[...].astype(jnp.float32)) * (1.0 + mod(0)) + mod(1)).astype(jnp.bfloat16)
        w_copy(0, layer).wait()

        def qkv_send(dest):
            return pltpu.make_async_remote_copy(msg.at[dest], kv.at[fresh, layer, pl.ds(row_own, block_rows), :], qkv_ss.at[dest], qkv_rs.at[my_head], device_id=dev(dest), device_id_type=MESH)

        def qkv_recv(src):
            rows = pl.ds(pl.multiple_of(device_row(src) * patch_rows + src % blocks * block_rows, block_rows), block_rows)
            return pltpu.make_async_remote_copy(msg.at[src], kv.at[fresh, layer, rows, :], qkv_ss.at[src], qkv_rs.at[src], device_id=dev(src), device_id_type=MESH)

        def make_group(group):
            first = group * blocks * head_dim // LANES
            for i in (1, 2, 0):
                lo = i * width + first * LANES
                cols = slice(lo, lo + group_tiles * LANES)
                bias_cols = slice(6 * width + cols.start, 6 * width + cols.stop)
                part = jnp.dot(normed, qkv_w[:, cols], preferred_element_type=jnp.float32) + bias_s[pl.ds(layer, 1), bias_cols]
                qkv_s[:, i * group_tiles * LANES:(i + 1) * group_tiles * LANES] = part.astype(jnp.bfloat16).astype(jnp.float32)

            def window(i, head, place):
                col = head * head_dim - first * LANES
                tile = min(col // LANES, group_tiles - 2)
                shift = (place - (col - tile * LANES)) % (2 * LANES)
                lo = (i * group_tiles + tile) * LANES
                part = qkv_s[:, lo:lo + 2 * LANES]
                return pltpu.roll(part, shift, 1) if shift else part

            for head in range(group * blocks, (group + 1) * blocks):
                block = jnp.where(lane2 < head_dim, window(1, head, 0),
                                  jnp.where(lane2 < 2 * head_dim, window(2, head, head_dim), window(0, head, 2 * head_dim)))
                msg[head] = block.astype(jnp.bfloat16)
            for dx in far_order:
                for dc in (1, 0):
                    dest = group * blocks + column(dx, dc)
                    if (dx, dc) == (0, 0):
                        @pl.when(own_group != group)
                        def _():
                            qkv_send(dest).start()

                        @pl.when(own_group == group)
                        def _():
                            kv[fresh, layer, pl.ds(row_own, block_rows), :] = msg[dest]
                    else:
                        qkv_send(dest).start()

        @pl.when(own_group == 1)
        def _():
            make_group(0)

        make_group(1)

        @pl.when(own_group == 0)
        def _():
            make_group(0)

        @pl.when(more)
        def _():
            w_copy(0, following).start()

        @pl.when(t == 0)
        def _():
            for kp in range(1, chips_y):
                @pl.when(kp > 2 * upper)
                def _():
                    rows = slice(kp * patch_rows, (kp + 1) * patch_rows)
                    stack = jnp.concatenate([old_s[0, layer, :, rows].astype(jnp.float32), old_s[1, layer, :, rows].astype(jnp.float32),
                                             jnp.zeros((2 * LANES - 2 * head_dim, patch_rows), jnp.float32)], axis=0)
                    kv[0, layer, rows, :] = stack.T.astype(jnp.bfloat16)

        for other in others:
            qkv_recv(member(*other)).wait_recv()

        def half_copy(half):
            rows = pl.ds(pl.multiple_of(half * half_rows, half_rows), half_rows)
            return pltpu.make_async_remote_copy(kv.at[fresh, layer, rows, :], kv.at[fresh, layer, rows, :], fwd_ss.at[layer], fwd_rs.at[layer], device_id=partner, device_id_type=MESH)

        def stored_copy():
            rows = pl.ds(half_rows, half_rows)
            return pltpu.make_async_remote_copy(kv.at[1, layer, rows, :], kv.at[1, layer, rows, :], fwd_ss.at[layer], fwd_rs.at[layer], device_id=partner, device_id_type=MESH)

        @pl.when(jnp.logical_and(upper == 0, t == 1))
        def _():
            stored_copy().wait_recv()

        @pl.when(upper == 0)
        def _():
            half_copy(0).start()

        @pl.when(upper == 1)
        def _():
            half_copy(0).wait_recv()

        def o_send(p, col):
            rows = pl.ds(pl.multiple_of((p % 2) * patch_rows + col * block_rows, block_rows), block_rows)
            dest = jnp.where(p == y, own_group, 1 - own_group) * blocks + col
            return pltpu.make_async_remote_copy(o_msg.at[rows, :], o_in.at[my_head], o_ss.at[dest], o_rs.at[my_head], device_id=(dp, p, col), device_id_type=MESH)

        def o_recv(src):
            return pltpu.make_async_remote_copy(o_msg.at[pl.ds(0, block_rows), :], o_in.at[src], o_ss.at[src], o_rs.at[src], device_id=dev(src), device_id_type=MESH)

        for flip in (1, 0):
            p = 2 * upper + (lane_row + flip) % 2
            q_rows = pl.ds(pl.multiple_of(p * patch_rows, patch_rows), patch_rows)
            q_part = pltpu.roll(kv[fresh, layer, q_rows, LANES:].astype(jnp.float32), 2 * LANES - 2 * head_dim, 1)
            q_part = jnp.where(lane1 < head_dim, q_part, 0.0).astype(jnp.bfloat16)
            slots = [jnp.where(kp <= p, fresh, 1 - fresh) for kp in range(chips_y)]
            scores = jnp.concatenate(
                [lax.dot_general(q_part, kv[slots[kp], layer, kp * patch_rows:(kp + 1) * patch_rows, :LANES], (((1,), (1,)), ((), ())), preferred_element_type=jnp.float32)
                 for kp in range(chips_y)], axis=1)
            top = jnp.max(scores, axis=-1, keepdims=True)
            e = jnp.exp2((scores - top) * factor)
            prob = (e * (1.0 / jnp.sum(e, axis=-1, keepdims=True))).astype(jnp.bfloat16)
            o = None
            for kp in range(chips_y):
                term = jnp.dot(prob[:, kp * patch_rows:(kp + 1) * patch_rows], kv[slots[kp], layer, kp * patch_rows:(kp + 1) * patch_rows, :], preferred_element_type=jnp.float32)
                o = term if o is None else o + term
            o_rows = pl.ds(pl.multiple_of((p % 2) * patch_rows, patch_rows), patch_rows)
            o_msg[o_rows, :] = pltpu.roll(o, 2 * LANES - head_dim, 1)[:, :LANES].astype(jnp.bfloat16)
            for dx in far_order:
                for dc in (1, 0):
                    if (flip, dx, dc) != (0, 0, 0):
                        o_send(p, column(dx, dc)).start()

        o_in[my_head] = o_msg[pl.ds(pl.multiple_of(lane_row * patch_rows + s * block_rows, block_rows), block_rows), :]

        @pl.when(jnp.logical_and(upper == 1, t == 0))
        def _():
            half_copy(1).start()

        for other in others:
            o_recv(member(*other)).wait_recv()

        pieces = [None] * tiles
        for head in range(heads):
            at = head * head_dim
            tile, off = at // LANES, at % LANES
            part = o_in[head].astype(jnp.float32)
            if off:
                part = pltpu.roll(part, off, 1)
            pieces[tile] = part if pieces[tile] is None else jnp.where(lane1 >= off, part, pieces[tile])
            if off + head_dim > LANES:
                pieces[tile + 1] = part
        attn = jnp.concatenate(pieces, axis=1).astype(jnp.bfloat16)
        w_copy(1, layer).wait()
        proj = jnp.dot(attn, o_w[...], preferred_element_type=jnp.float32) + bias(9, 10)

        @pl.when(more)
        def _():
            w_copy(1, following).start()

        residual = hid_s[...].astype(jnp.float32) + mod(2) * proj
        mlp_in = (normalize(residual) * (1.0 + mod(3)) + mod(4)).astype(jnp.bfloat16)
        w_copy(2, layer).wait()
        for i in range(4):
            cols = slice(i * width, (i + 1) * width)
            up = jnp.dot(mlp_in, up_w[:, cols], preferred_element_type=jnp.float32) + bias(10 + i, 11 + i)
            mid_s[:, cols] = jax.nn.gelu(up, approximate=True).astype(jnp.bfloat16)

        @pl.when(more)
        def _():
            w_copy(2, following).start()

        w_copy(3, layer).wait()
        down = jnp.dot(mid_s[...], down_w[...], preferred_element_type=jnp.float32) + bias(14, 15)
        hid_s[...] = (residual + mod(5) * down).astype(jnp.bfloat16)

        @pl.when(more)
        def _():
            w_copy(3, following).start()

        @pl.when(layer == layers - 1)
        def _():
            scale_out = fmod_s[pl.ds(t, 1), :width]
            shift_out = fmod_s[pl.ds(t, 1), width:]
            out_rows = (normalize(hid_s[...].astype(jnp.float32)) * (1.0 + scale_out) + shift_out).astype(jnp.bfloat16)
            velocity = lax.dot_general(w_out_ref[...], out_rows, (((1,), (1,)), ((), ())), preferred_element_type=jnp.float32)
            lat_s[...] = lat_s[...] + step_ref[t] * velocity

        for other in others:
            qkv_send(member(*other)).wait_send()
            flip, dx, dc = other
            o_send(2 * upper + (lane_row + flip) % 2, column(dx, dc)).wait_send()

        @pl.when(upper == 0)
        def _():
            half_copy(0).wait_send()

        @pl.when(jnp.logical_and(upper == 1, t == 0))
        def _():
            half_copy(1).wait_send()

        return carry

    lax.fori_loop(0, 2 * layers, layer_pass, 0)

    def out_send(k):
        row = (y + k) % chips_y
        return pltpu.make_async_remote_copy(lat_s, out_in.at[y], out_ss.at[row], out_rs.at[y], device_id=(dp, row, s), device_id_type=MESH)

    def out_recv(k):
        row = (y + k) % chips_y
        return pltpu.make_async_remote_copy(lat_s, out_in.at[row], out_ss.at[row], out_rs.at[row], device_id=(dp, row, s), device_id_type=MESH)

    for k in range(1, chips_y):
        out_send(k).start()
    out_in[y] = lat_s[...]
    for k in range(1, chips_y):
        out_recv(k).wait_recv()
    out_ref[...] = out_in[...]
    for k in range(1, chips_y):
        out_send(k).wait_send()


def solution(mesh):
    chips_y = mesh.shape["pp"]
    chips_x = mesh.shape["sp"] // 2
    row_spec = P("dp", "sp", None)
    full_spec = P()
    buf_spec = P("dp", None, None, None)
    in_specs = (row_spec, P(None, "sp", None), P("dp", None), P("dp"), full_spec, full_spec, full_spec, full_spec, full_spec, full_spec, full_spec, full_spec, full_spec, full_spec, buf_spec, buf_spec)

    def device_fn(latent_in, pos_embed, condition, step_size, w_in, w_ada, w_qkv, w_o, w_up, w_down, b_layer, w_fa, b_fa, w_out, k_old, v_old):
        patches, block_rows, latent_dim = latent_in.shape
        layers, width = w_qkv.shape[:2]
        tokens, heads, head_dim = k_old.shape[1:]
        members = 4 * chips_x
        parts = members // layers
        ada_tiles = -(-(w_ada.shape[2] // LANES) // parts)
        fa_tiles = -(-(w_fa.shape[1] // LANES) // members)
        ada_rows = 2 * (ada_tiles + fa_tiles)
        half_rows = 2 * block_rows * 2 * chips_x
        group_cols = -(-(heads // 2 * head_dim) // LANES) * LANES
        dims = (chips_x, chips_y, layers, block_rows, width, heads, head_dim)
        bf16, f32 = jnp.bfloat16, jnp.float32
        vmem = pl.BlockSpec(memory_space=pltpu.VMEM)
        hbm = pl.BlockSpec(memory_space=pl.ANY)
        dma = pltpu.SemaphoreType.DMA
        latent_t = jnp.transpose(latent_in, (0, 2, 1))
        k_t = jnp.transpose(k_old, (0, 2, 3, 1))
        v_t = jnp.transpose(v_old, (0, 2, 3, 1))
        result = pl.pallas_call(
            functools.partial(kernel, dims),
            out_shape=jax.ShapeDtypeStruct(latent_t.shape, f32),
            in_specs=[vmem, vmem, pl.BlockSpec(memory_space=pltpu.SMEM), vmem, vmem, vmem] + [hbm] * 10,
            out_specs=vmem,
            scratch_shapes=[
                pltpu.VMEM((width, ada_tiles * LANES), bf16),
                pltpu.VMEM((width, fa_tiles * LANES), bf16),
                pltpu.VMEM(w_qkv.shape[1:], bf16),
                pltpu.VMEM(w_o.shape[1:], bf16),
                pltpu.VMEM(w_up.shape[1:], bf16),
                pltpu.VMEM(w_down.shape[1:], bf16),
                pltpu.VMEM((2, layers, tokens, 2 * LANES), bf16),
                pltpu.VMEM((2, layers, head_dim, tokens), bf16),
                pltpu.VMEM((block_rows, 3 * group_cols), f32),
                pltpu.VMEM((members, block_rows, 2 * LANES), bf16),
                pltpu.VMEM((half_rows, LANES), bf16),
                pltpu.VMEM((members, block_rows, LANES), bf16),
                pltpu.VMEM((ada_rows, LANES), f32),
                pltpu.VMEM((members, ada_rows, LANES), f32),
                pltpu.VMEM((2 * layers, w_ada.shape[2]), f32),
                pltpu.VMEM((2, w_fa.shape[1]), f32),
                pltpu.VMEM(b_layer.shape, bf16),
                pltpu.VMEM(b_layer.shape, f32),
                pltpu.VMEM((block_rows, width), bf16),
                pltpu.VMEM((latent_dim, block_rows), f32),
                pltpu.VMEM((block_rows, width), bf16),
                pltpu.VMEM((block_rows, w_up.shape[2]), bf16),
                pltpu.VMEM((patches, latent_dim, block_rows), f32),
                dma((4,)), dma((6,)), dma((members,)), dma((members,)), dma((members,)), dma((members,)), dma((members,)), dma((members,)),
                dma((layers,)), dma((layers,)), dma((chips_y,)), dma((chips_y,)),
            ],
            compiler_params=pltpu.CompilerParams(collective_id=0, has_side_effects=True, vmem_limit_bytes=60 * 1024 * 1024),
        )(latent_t, condition, step_size, w_in, b_fa[None, :], w_out.T, pos_embed, b_layer, k_t, v_t, w_ada, w_fa, w_qkv, w_o, w_up, w_down)
        return jnp.transpose(result, (0, 2, 1))

    return jax.shard_map(device_fn, mesh=mesh, in_specs=in_specs, out_specs=row_spec, check_vma=False)
```

```python
import functools

import jax
import jax.numpy as jnp
from jax import lax
from jax.experimental import pallas as pl
from jax.experimental.pallas import tpu as pltpu
from jax.sharding import PartitionSpec as P

LN_EPS = 1e-6
LANES = 128
LOG2_E = 1.4426950408889634
MESH = pl.DeviceIdType.MESH


def normalize(hidden):
    mean_val = jnp.mean(hidden, axis=-1, keepdims=True)
    centered = hidden - mean_val
    var_val = jnp.mean(centered * centered, axis=-1, keepdims=True)
    return centered * lax.rsqrt(var_val + LN_EPS)


def kernel(dims, cond_ref, step_ref, w_in_ref, b_fa_ref, w_out_ref,
           latent_hbm, pos_hbm, b_layer_hbm, k_hbm, v_hbm, w_ada_hbm, w_fa_hbm, w_qkv_hbm, w_o_hbm, w_up_hbm, w_down_hbm,
           out_ref,
           ada_w, fa_w, qkv_w, o_w, up_w, down_w, kv, old_s, msg, o_msg, o_in, first_msg, first_in, ada_msg, ada_in,
           mod_s, fmod_s, bias_in, bias_s, hid_s, lat_s, pos_s,
           w_sem, load_sem, first_ss, first_rs, ada_ss, ada_rs, qkv_ss, qkv_rs, o_ss, o_rs, fwd_ss, fwd_rs, out_ss, out_rs):
    (chips_x, chips_y, layers, block_rows, width, heads, head_dim) = dims
    blocks = 2 * chips_x
    patch_rows = block_rows * blocks
    half_rows = 2 * patch_rows
    members = 2 * blocks
    far_order = sorted(range(chips_x), key=lambda d: -min(d, chips_x - d))
    dp = lax.axis_index("dp")
    y = lax.axis_index("pp")
    s = lax.axis_index("sp")
    x = s // 2
    core = s % 2
    upper = y // 2
    lane_row = y % 2
    own_group = jnp.where(upper == 0, lane_row, 1 - lane_row)
    my_head = own_group * blocks + s
    row_own = pl.multiple_of(y * patch_rows + s * block_rows, block_rows)

    def group_row(group):
        return jnp.where(upper == 0, group, chips_y - 1 - group)

    def column(dx, dc):
        return 2 * ((x + dx) % chips_x) + (core + dc) % 2

    def device_row(head):
        return group_row(head // blocks)

    def dev(head):
        return (dp, device_row(head), head % blocks)

    others = [(flip, dx, dc) for flip in (1, 0) for dx in far_order for dc in (1, 0) if (flip, dx, dc) != (0, 0, 0)]

    def member(flip, dx, dc):
        return (own_group + flip) % 2 * blocks + column(dx, dc)

    partner = (dp, chips_y - 1 - y, s)

    ada_tiles = ada_w.shape[2] // LANES
    ada_total = w_ada_hbm.shape[2] // LANES
    fa_tiles = fa_w.shape[1] // LANES
    fa_total = w_fa_hbm.shape[1] // LANES

    ada_col = pl.multiple_of(jnp.minimum(ada_tiles * my_head, ada_total - ada_tiles) * LANES, LANES)
    fa_col = pl.multiple_of(jnp.minimum(fa_tiles * my_head, fa_total - fa_tiles) * LANES, LANES)
    ada_cols = pl.ds(ada_col, ada_w.shape[2])
    ada_copy = pltpu.make_async_copy(w_ada_hbm.at[0, :, ada_cols], ada_w.at[0], load_sem.at[0])
    ada_copy.start()
    rest_copy = pltpu.make_async_copy(w_ada_hbm.at[1:, :, ada_cols], ada_w.at[1:], load_sem.at[6])
    rest_copy.start()
    fa_copy = pltpu.make_async_copy(w_fa_hbm.at[:, pl.ds(fa_col, fa_w.shape[1])], fa_w, load_sem.at[1])
    fa_copy.start()
    bias_copy = pltpu.make_async_copy(b_layer_hbm, bias_in, load_sem.at[2])
    bias_copy.start()
    pos_copy = pltpu.make_async_copy(pos_hbm.at[y], pos_s, load_sem.at[3])
    pos_copy.start()
    lat_copy = pltpu.make_async_copy(latent_hbm.at[y], lat_s, load_sem.at[7])
    lat_copy.start()

    def w_copy(which, layer):
        src, dst = ((w_qkv_hbm, qkv_w), (w_o_hbm, o_w), (w_up_hbm, up_w), (w_down_hbm, down_w))[which]
        return pltpu.make_async_copy(src.at[layer], dst, w_sem.at[which])

    k_copy = pltpu.make_async_copy(k_hbm.at[:, my_head], old_s.at[0], load_sem.at[4])
    v_copy = pltpu.make_async_copy(v_hbm.at[:, my_head], old_s.at[1], load_sem.at[5])

    barrier = pltpu.get_barrier_semaphore()
    for flip, dx, dc in others:
        pl.semaphore_signal(barrier, inc=1, device_id=dev(member(flip, dx, dc)), device_id_type=MESH)
    for k in range(2):
        pl.semaphore_signal(barrier, inc=1, device_id=(dp, (1 - upper) * 2 + k, s), device_id_type=MESH)

    cond = cond_ref[...].astype(jnp.float32)
    act = (cond * jax.nn.sigmoid(cond)).astype(jnp.bfloat16)

    def put_rows(msg_ref, row, value, count):
        for t in range(2):
            for i in range(count):
                at = row + t * count + i
                msg_ref[at:at + 1, :] = value[t:t + 1, i * LANES:(i + 1) * LANES]

    ada_copy.wait()
    w_copy(0, 0).start()
    put_rows(first_msg, 0, jnp.dot(act, ada_w[0], preferred_element_type=jnp.float32), ada_tiles)

    def first_copy(other, src_side):
        peer = member(*other)
        slot = peer if src_side else my_head
        return pltpu.make_async_remote_copy(first_msg, first_in.at[slot], first_ss.at[peer], first_rs.at[slot], device_id=dev(peer), device_id_type=MESH)

    def late_copy(other, src_side):
        peer = member(*other)
        slot = peer if src_side else my_head
        return pltpu.make_async_remote_copy(ada_msg, ada_in.at[slot], ada_ss.at[peer], ada_rs.at[slot], device_id=dev(peer), device_id_type=MESH)

    pl.semaphore_wait(barrier, members + 1)
    for other in others:
        first_copy(other, False).start()
    first_in[my_head] = first_msg[...]
    rest_copy.wait()
    for layer in range(1, layers):
        put_rows(ada_msg, (layer - 1) * 2 * ada_tiles, jnp.dot(act, ada_w[layer], preferred_element_type=jnp.float32), ada_tiles)
    fa_copy.wait()
    put_rows(ada_msg, (layers - 1) * 2 * ada_tiles, jnp.dot(act, fa_w[...], preferred_element_type=jnp.float32), fa_tiles)
    for other in others:
        late_copy(other, False).start()
    ada_in[my_head] = ada_msg[...]
    k_copy.start()
    v_copy.start()
    for which in range(1, 4):
        w_copy(which, 0).start()
    bias_copy.wait()
    bias_s[...] = bias_in[...].astype(jnp.float32)
    lat_copy.wait()
    pos_copy.wait()

    def take_rows(in_ref, base, layer):
        for t in range(2):
            for tile in range(ada_total):
                part = min(tile // ada_tiles, -(-ada_total // ada_tiles) - 1)
                first = min(ada_tiles * part, ada_total - ada_tiles)
                row = base + t * ada_tiles + tile - first
                cols = slice(tile * LANES, (tile + 1) * LANES)
                mod_s[t * layers + layer:t * layers + layer + 1, cols] = in_ref[part, row:row + 1, :] + bias_s[layer:layer + 1, cols]

    for other in others:
        first_copy(other, True).wait_recv()
    take_rows(first_in, 0, 0)

    lane2 = lax.broadcasted_iota(jnp.int32, (1, 2 * LANES), 1)
    lane1 = lax.broadcasted_iota(jnp.int32, (1, LANES), 1)
    factor = LOG2_E * head_dim ** -0.5
    tiles = width // LANES
    group_tiles = -(-(blocks * head_dim) // LANES)

    def layer_pass(it, carry):
        t = it // layers
        layer = it % layers
        following = (it + 1) % layers
        more = it + 1 < 2 * layers
        fresh = 1 - t
        bias = lambda lo, hi: bias_s[pl.ds(layer, 1), lo * width:hi * width]
        mod = lambda i: mod_s[pl.ds(it, 1), i * width:(i + 1) * width]

        @pl.when(layer == 0)
        def _():
            emb = lax.dot_general(lat_s[...].astype(jnp.bfloat16), w_in_ref[...], (((0,), (0,)), ((), ())), preferred_element_type=jnp.float32)
            hid_s[...] = (emb + pos_s[...].astype(jnp.float32)).astype(jnp.bfloat16)

        normed = (normalize(hid_s[...].astype(jnp.float32)) * (1.0 + mod(0)) + mod(1)).astype(jnp.bfloat16)
        w_copy(0, layer).wait()

        def qkv_send(dest):
            return pltpu.make_async_remote_copy(msg.at[dest], kv.at[fresh, layer, pl.ds(row_own, block_rows), :], qkv_ss.at[dest], qkv_rs.at[my_head], device_id=dev(dest), device_id_type=MESH)

        def qkv_recv(src):
            rows = pl.ds(pl.multiple_of(device_row(src) * patch_rows + src % blocks * block_rows, block_rows), block_rows)
            return pltpu.make_async_remote_copy(msg.at[src], kv.at[fresh, layer, rows, :], qkv_ss.at[src], qkv_rs.at[src], device_id=dev(src), device_id_type=MESH)

        far = 1 - own_group
        wide = group_tiles * LANES
        narrow = width - wide
        far_col = far * narrow
        near_col = (1 - far) * wide
        shift_unit = blocks * head_dim - narrow

        def columns(i, start, size):
            cols = pl.ds(pl.multiple_of(i * width + start, LANES), size)
            bias_cols = pl.ds(pl.multiple_of((6 + i) * width + start, LANES), size)
            part = jnp.dot(normed, qkv_w[:, cols], preferred_element_type=jnp.float32) + bias_s[pl.ds(layer, 1), bias_cols]
            return part.astype(jnp.bfloat16).astype(jnp.float32)

        def pack_group(group, parts):
            parts = [jnp.where(group == 1, pltpu.roll(part, wide - shift_unit, 1), part) for part in parts]

            def window(i, col, place):
                tile = min(col // LANES, group_tiles - 2)
                shift = (place - (col - tile * LANES)) % (2 * LANES)
                part = parts[i][:, tile * LANES:(tile + 2) * LANES]
                return pltpu.roll(part, shift, 1) if shift else part

            for k in range(blocks):
                col = k * head_dim
                block = jnp.where(lane2 < head_dim, window(1, col, 0),
                                  jnp.where(lane2 < 2 * head_dim, window(2, col, head_dim), window(0, col, 2 * head_dim)))
                msg[group * blocks + k] = block.astype(jnp.bfloat16)

        firsts = [columns(i, far_col, wide) for i in range(3)]
        pack_group(far, firsts)
        for dx in far_order:
            for dc in (1, 0):
                qkv_send(far * blocks + column(dx, dc)).start()
        seconds = [columns(i, near_col, narrow) for i in range(3)]
        pack_group(own_group, [jnp.where(far == 0, jnp.concatenate([first[:, narrow:], second], axis=1), jnp.concatenate([second, first[:, :wide - narrow]], axis=1))
                               for first, second in zip(firsts, seconds)])
        for dx in far_order:
            for dc in (1, 0):
                if (dx, dc) != (0, 0):
                    qkv_send(own_group * blocks + column(dx, dc)).start()
        kv[fresh, layer, pl.ds(row_own, block_rows), :] = msg[my_head]

        @pl.when(more)
        def _():
            w_copy(0, following).start()

        @pl.when(it == 0)
        def _():
            k_copy.wait()
            v_copy.wait()

        @pl.when(t == 0)
        def _():
            for kp in range(1, chips_y):
                @pl.when(kp > 2 * upper)
                def _():
                    rows = slice(kp * patch_rows, (kp + 1) * patch_rows)
                    stack = jnp.concatenate([old_s[0, layer, :, rows].astype(jnp.float32), old_s[1, layer, :, rows].astype(jnp.float32),
                                             jnp.zeros((2 * LANES - 2 * head_dim, patch_rows), jnp.float32)], axis=0)
                    kv[0, layer, rows, :] = stack.T.astype(jnp.bfloat16)

        for other in others:
            qkv_recv(member(*other)).wait_recv()

        def half_copy(half):
            rows = pl.ds(pl.multiple_of(half * half_rows, half_rows), half_rows)
            return pltpu.make_async_remote_copy(kv.at[fresh, layer, rows, :], kv.at[fresh, layer, rows, :], fwd_ss.at[layer], fwd_rs.at[layer], device_id=partner, device_id_type=MESH)

        def stored_copy():
            rows = pl.ds(half_rows, half_rows)
            return pltpu.make_async_remote_copy(kv.at[1, layer, rows, :], kv.at[1, layer, rows, :], fwd_ss.at[layer], fwd_rs.at[layer], device_id=partner, device_id_type=MESH)

        @pl.when(jnp.logical_and(upper == 0, t == 1))
        def _():
            stored_copy().wait_recv()

        @pl.when(upper == 0)
        def _():
            half_copy(0).start()

        @pl.when(upper == 1)
        def _():
            half_copy(0).wait_recv()

        def o_send(p, col):
            rows = pl.ds(pl.multiple_of((p % 2) * patch_rows + col * block_rows, block_rows), block_rows)
            dest = jnp.where(p == y, own_group, 1 - own_group) * blocks + col
            return pltpu.make_async_remote_copy(o_msg.at[rows, :], o_in.at[my_head], o_ss.at[dest], o_rs.at[my_head], device_id=(dp, p, col), device_id_type=MESH)

        def o_recv(src):
            return pltpu.make_async_remote_copy(o_msg.at[pl.ds(0, block_rows), :], o_in.at[src], o_ss.at[src], o_rs.at[src], device_id=dev(src), device_id_type=MESH)

        pair = 2 * block_rows

        def queries(flip, dxs):
            p = 2 * upper + (lane_row + flip) % 2
            offsets = [(x + dx) % chips_x * pair for dx in dxs]
            if len(dxs) == chips_x:
                q_part = kv[fresh, layer, pl.ds(pl.multiple_of(p * patch_rows, patch_rows), patch_rows), LANES:]
            else:
                q_part = jnp.concatenate([kv[fresh, layer, pl.ds(pl.multiple_of(p * patch_rows + at, pair), pair), LANES:] for at in offsets], axis=0)
            q_part = pltpu.roll(q_part.astype(jnp.float32), 2 * LANES - 2 * head_dim, 1)
            return jnp.where(lane1 < head_dim, q_part, 0.0).astype(jnp.bfloat16)

        def blocks_of(flip, lanes):
            p = 2 * upper + (lane_row + flip) % 2
            return [kv[jnp.where(kp <= p, fresh, 1 - fresh), layer, kp * patch_rows:(kp + 1) * patch_rows, :lanes] for kp in range(chips_y)]

        def score(flip, dxs):
            q_part = queries(flip, dxs)
            return [lax.dot_general(q_part, block, (((1,), (1,)), ((), ())), preferred_element_type=jnp.float32) for block in blocks_of(flip, LANES)]

        def probs(scores):
            scores = jnp.concatenate(scores, axis=1)
            top = jnp.max(scores, axis=-1, keepdims=True)
            e = jnp.exp2((scores - top) * factor)
            return (e * (1.0 / jnp.sum(e, axis=-1, keepdims=True))).astype(jnp.bfloat16)

        def values(flip, dxs, prob):
            p = 2 * upper + (lane_row + flip) % 2
            o = None
            for kp, block in enumerate(blocks_of(flip, 2 * LANES)):
                term = jnp.dot(prob[:, kp * patch_rows:(kp + 1) * patch_rows], block, preferred_element_type=jnp.float32)
                o = term if o is None else o + term
            o = pltpu.roll(o, 2 * LANES - head_dim, 1)[:, :LANES].astype(jnp.bfloat16)
            if len(dxs) == chips_x:
                o_msg[pl.ds(pl.multiple_of((p % 2) * patch_rows, patch_rows), patch_rows), :] = o
            else:
                for i, dx in enumerate(dxs):
                    o_msg[pl.ds(pl.multiple_of((p % 2) * patch_rows + (x + dx) % chips_x * pair, pair), pair), :] = o[i * pair:(i + 1) * pair]

        def send_rows(flip, dxs):
            p = 2 * upper + (lane_row + flip) % 2
            for dx in dxs:
                for dc in (1, 0):
                    if (flip, dx, dc) != (0, 0, 0):
                        o_send(p, column(dx, dc)).start()

        chunks = [(flip, far_order) for flip in (1, 0)]
        all_scores = [score(*chunk) for chunk in chunks]
        all_probs = [probs(scores) for scores in all_scores]
        for (flip, dxs), prob in zip(chunks, all_probs):
            values(flip, dxs, prob)
        for flip, dxs in chunks:
            send_rows(flip, dxs)

        o_in[my_head] = o_msg[pl.ds(pl.multiple_of(lane_row * patch_rows + s * block_rows, block_rows), block_rows), :]

        @pl.when(jnp.logical_and(upper == 1, t == 0))
        def _():
            half_copy(1).start()

        @pl.when(it == 0)
        def _():
            for other in others:
                late_copy(other, True).wait_recv()
            for late in range(1, layers):
                take_rows(ada_in, (late - 1) * 2 * ada_tiles, late)
            for step in range(2):
                for tile in range(fa_total):
                    row = (layers - 1) * 2 * ada_tiles + step * fa_tiles + tile % fa_tiles
                    cols = slice(tile * LANES, (tile + 1) * LANES)
                    fmod_s[step:step + 1, cols] = ada_in[tile // fa_tiles, row:row + 1, :] + b_fa_ref[cols].astype(jnp.float32).reshape(1, LANES)
            for other in others:
                first_copy(other, False).wait_send()
                late_copy(other, False).wait_send()

        for other in others:
            o_recv(member(*other)).wait_recv()

        pieces = [None] * tiles
        for head in range(heads):
            at = head * head_dim
            tile, off = at // LANES, at % LANES
            part = o_in[head].astype(jnp.float32)
            if off:
                part = pltpu.roll(part, off, 1)
            pieces[tile] = part if pieces[tile] is None else jnp.where(lane1 >= off, part, pieces[tile])
            if off + head_dim > LANES:
                pieces[tile + 1] = part
        attn = jnp.concatenate(pieces, axis=1).astype(jnp.bfloat16)
        w_copy(1, layer).wait()
        proj = jnp.dot(attn, o_w[...], preferred_element_type=jnp.float32) + bias(9, 10)

        @pl.when(more)
        def _():
            w_copy(1, following).start()

        residual = hid_s[...].astype(jnp.float32) + mod(2) * proj
        mlp_in = (normalize(residual) * (1.0 + mod(3)) + mod(4)).astype(jnp.bfloat16)
        w_copy(2, layer).wait()
        up_cols = up_w.shape[1] // 4
        w_copy(3, layer).wait()
        down = bias(14, 15)
        for i in range(4):
            cols = slice(i * up_cols, (i + 1) * up_cols)
            up_bias = bias_s[pl.ds(layer, 1), 10 * width + i * up_cols:10 * width + (i + 1) * up_cols]
            up = jnp.dot(mlp_in, up_w[:, cols], preferred_element_type=jnp.float32) + up_bias
            mid = jax.nn.gelu(up, approximate=True).astype(jnp.bfloat16)
            down = down + jnp.dot(mid, down_w[cols, :], preferred_element_type=jnp.float32)

        @pl.when(more)
        def _():
            w_copy(2, following).start()

        hid_s[...] = (residual + mod(5) * down).astype(jnp.bfloat16)

        @pl.when(more)
        def _():
            w_copy(3, following).start()

        @pl.when(layer == layers - 1)
        def _():
            scale_out = fmod_s[pl.ds(t, 1), :width]
            shift_out = fmod_s[pl.ds(t, 1), width:]
            out_rows = (normalize(hid_s[...].astype(jnp.float32)) * (1.0 + scale_out) + shift_out).astype(jnp.bfloat16)
            velocity = lax.dot_general(w_out_ref[...], out_rows, (((1,), (1,)), ((), ())), preferred_element_type=jnp.float32)
            lat_s[...] = lat_s[...] + step_ref[t] * velocity

        for other in others:
            qkv_send(member(*other)).wait_send()
            flip, dx, dc = other
            o_send(2 * upper + (lane_row + flip) % 2, column(dx, dc)).wait_send()

        @pl.when(upper == 0)
        def _():
            half_copy(0).wait_send()

        @pl.when(jnp.logical_and(upper == 1, t == 0))
        def _():
            half_copy(1).wait_send()

        return carry

    lax.fori_loop(0, 2 * layers, layer_pass, 0)

    def out_copy(k, src_side):
        row = (y + k) % chips_y
        slot = row if src_side else y
        return pltpu.make_async_remote_copy(lat_s, out_ref.at[slot], out_ss.at[row], out_rs.at[slot], device_id=(dp, row, s), device_id_type=MESH)

    for k in range(1, chips_y):
        out_copy(k, False).start()
    own_copy = pltpu.make_async_copy(lat_s, out_ref.at[y], load_sem.at[0])
    own_copy.start()
    for k in range(1, chips_y):
        out_copy(k, True).wait_recv()
    own_copy.wait()
    for k in range(1, chips_y):
        out_copy(k, False).wait_send()


def solution(mesh):
    chips_y = mesh.shape["pp"]
    chips_x = mesh.shape["sp"] // 2
    row_spec = P("dp", "sp", None)
    full_spec = P()
    buf_spec = P("dp", None, None, None)
    in_specs = (row_spec, P(None, "sp", None), P("dp", None), P("dp"), full_spec, full_spec, full_spec, full_spec, full_spec, full_spec, full_spec, full_spec, full_spec, full_spec, buf_spec, buf_spec)

    def device_fn(latent_in, pos_embed, condition, step_size, w_in, w_ada, w_qkv, w_o, w_up, w_down, b_layer, w_fa, b_fa, w_out, k_old, v_old):
        patches, block_rows, latent_dim = latent_in.shape
        layers, width = w_qkv.shape[:2]
        tokens, heads, head_dim = k_old.shape[1:]
        members = 4 * chips_x
        ada_tiles = -(-(w_ada.shape[2] // LANES) // members)
        fa_tiles = -(-(w_fa.shape[1] // LANES) // members)
        ada_rows = 2 * ((layers - 1) * ada_tiles + fa_tiles)
        half_rows = 2 * block_rows * 2 * chips_x
        dims = (chips_x, chips_y, layers, block_rows, width, heads, head_dim)
        bf16, f32 = jnp.bfloat16, jnp.float32
        vmem = pl.BlockSpec(memory_space=pltpu.VMEM)
        hbm = pl.BlockSpec(memory_space=pl.ANY)
        dma = pltpu.SemaphoreType.DMA
        latent_t = jnp.transpose(latent_in, (0, 2, 1))
        k_t = jnp.transpose(k_old, (0, 2, 3, 1))
        v_t = jnp.transpose(v_old, (0, 2, 3, 1))
        result = pl.pallas_call(
            functools.partial(kernel, dims),
            out_shape=jax.ShapeDtypeStruct(latent_t.shape, f32),
            in_specs=[vmem, pl.BlockSpec(memory_space=pltpu.SMEM), vmem, vmem, vmem] + [hbm] * 11,
            out_specs=hbm,
            scratch_shapes=[
                pltpu.VMEM((layers, width, ada_tiles * LANES), bf16),
                pltpu.VMEM((width, fa_tiles * LANES), bf16),
                pltpu.VMEM(w_qkv.shape[1:], bf16),
                pltpu.VMEM(w_o.shape[1:], bf16),
                pltpu.VMEM(w_up.shape[1:], bf16),
                pltpu.VMEM(w_down.shape[1:], bf16),
                pltpu.VMEM((2, layers, tokens, 2 * LANES), bf16),
                pltpu.VMEM((2, layers, head_dim, tokens), bf16),
                pltpu.VMEM((members, block_rows, 2 * LANES), bf16),
                pltpu.VMEM((half_rows, LANES), bf16),
                pltpu.VMEM((members, block_rows, LANES), bf16),
                pltpu.VMEM((2 * ada_tiles, LANES), f32),
                pltpu.VMEM((members, 2 * ada_tiles, LANES), f32),
                pltpu.VMEM((ada_rows, LANES), f32),
                pltpu.VMEM((members, ada_rows, LANES), f32),
                pltpu.VMEM((2 * layers, w_ada.shape[2]), f32),
                pltpu.VMEM((2, w_fa.shape[1]), f32),
                pltpu.VMEM(b_layer.shape, bf16),
                pltpu.VMEM(b_layer.shape, f32),
                pltpu.VMEM((block_rows, width), bf16),
                pltpu.VMEM((latent_dim, block_rows), f32),
                pltpu.VMEM((block_rows, width), bf16),
                dma((4,)), dma((8,)), dma((members,)), dma((members,)), dma((members,)), dma((members,)), dma((members,)), dma((members,)), dma((members,)), dma((members,)),
                dma((layers,)), dma((layers,)), dma((chips_y,)), dma((chips_y,)),
            ],
            compiler_params=pltpu.CompilerParams(collective_id=0, has_side_effects=True, vmem_limit_bytes=60 * 1024 * 1024),
        )(condition, step_size, w_in, b_fa, w_out.T, latent_t, pos_embed, b_layer, k_t, v_t, w_ada, w_fa, w_qkv, w_o, w_up, w_down)
        return jnp.transpose(result, (0, 2, 1))

    return jax.shard_map(device_fn, mesh=mesh, in_specs=in_specs, out_specs=row_spec, check_vma=False)
```

```python
import functools

import jax
import jax.numpy as jnp
from jax import lax
from jax.experimental import pallas as pl
from jax.experimental.pallas import tpu as pltpu
from jax.sharding import PartitionSpec as P

LN_EPS = 1e-6
LANES = 128
LOG2_E = 1.4426950408889634
MESH = pl.DeviceIdType.MESH


def normalize(hidden):
    mean_val = jnp.mean(hidden, axis=-1, keepdims=True)
    centered = hidden - mean_val
    var_val = jnp.mean(centered * centered, axis=-1, keepdims=True)
    return centered * lax.rsqrt(var_val + LN_EPS)


def kernel(dims, cond_ref, step_ref, w_in_ref, b_fa_ref, w_out_ref,
           latent_hbm, pos_hbm, b_layer_hbm, k_hbm, v_hbm, w_ada_hbm, w_fa_hbm, w_qkv_hbm, w_o_hbm, w_up_hbm, w_down_hbm,
           out_ref,
           head_w, ada_w, fa_w, qkv_w, o_w, up_w, down_w, kv, old_s, msg, o_msg, o_in, ada_msg, ada_in,
           mod_s, fmod_s, bias_in, bias_s, hid_s, lat_s, pos_s,
           w_sem, load_sem, ada_ss, ada_rs, qkv_ss, qkv_rs, o_ss, o_rs, fwd_ss, fwd_rs, out_ss, out_rs):
    (chips_x, chips_y, layers, block_rows, width, heads, head_dim) = dims
    blocks = 2 * chips_x
    patch_rows = block_rows * blocks
    half_rows = 2 * patch_rows
    members = 2 * blocks
    far_order = sorted(range(chips_x), key=lambda d: -min(d, chips_x - d))
    dp = lax.axis_index("dp")
    y = lax.axis_index("pp")
    s = lax.axis_index("sp")
    x = s // 2
    core = s % 2
    upper = y // 2
    lane_row = y % 2
    own_group = jnp.where(upper == 0, lane_row, 1 - lane_row)
    my_head = own_group * blocks + s
    row_own = pl.multiple_of(y * patch_rows + s * block_rows, block_rows)

    def group_row(group):
        return jnp.where(upper == 0, group, chips_y - 1 - group)

    def column(dx, dc):
        return 2 * ((x + dx) % chips_x) + (core + dc) % 2

    def device_row(head):
        return group_row(head // blocks)

    def dev(head):
        return (dp, device_row(head), head % blocks)

    others = [(flip, dx, dc) for flip in (1, 0) for dx in far_order for dc in (1, 0) if (flip, dx, dc) != (0, 0, 0)]

    def member(flip, dx, dc):
        return (own_group + flip) % 2 * blocks + column(dx, dc)

    partner = (dp, chips_y - 1 - y, s)

    ada_tiles = ada_w.shape[2] // LANES
    ada_total = w_ada_hbm.shape[2] // LANES
    fa_tiles = fa_w.shape[1] // LANES
    fa_total = w_fa_hbm.shape[1] // LANES

    ada_col = pl.multiple_of(jnp.minimum(ada_tiles * my_head, ada_total - ada_tiles) * LANES, LANES)
    fa_col = pl.multiple_of(jnp.minimum(fa_tiles * my_head, fa_total - fa_tiles) * LANES, LANES)
    head_copy = pltpu.make_async_copy(w_ada_hbm.at[0, :, pl.ds(0, head_w.shape[1])], head_w, load_sem.at[0])
    head_copy.start()
    bias_copy = pltpu.make_async_copy(b_layer_hbm, bias_in, load_sem.at[2])
    bias_copy.start()
    pos_copy = pltpu.make_async_copy(pos_hbm.at[y], pos_s, load_sem.at[3])
    pos_copy.start()
    lat_copy = pltpu.make_async_copy(latent_hbm.at[y], lat_s, load_sem.at[7])
    lat_copy.start()
    ada_copy = pltpu.make_async_copy(w_ada_hbm.at[:, :, pl.ds(ada_col, ada_w.shape[2])], ada_w, load_sem.at[6])
    fa_copy = pltpu.make_async_copy(w_fa_hbm.at[:, pl.ds(fa_col, fa_w.shape[1])], fa_w, load_sem.at[1])
    k_copy = pltpu.make_async_copy(k_hbm.at[:, my_head], old_s.at[0], load_sem.at[4])
    v_copy = pltpu.make_async_copy(v_hbm.at[:, my_head], old_s.at[1], load_sem.at[5])

    def w_copy(which, layer):
        src, dst = ((w_qkv_hbm, qkv_w), (w_o_hbm, o_w), (w_up_hbm, up_w), (w_down_hbm, down_w))[which]
        return pltpu.make_async_copy(src.at[layer], dst, w_sem.at[which])

    w_copy(0, 0).start()

    barrier = pltpu.get_barrier_semaphore()
    for flip, dx, dc in others:
        pl.semaphore_signal(barrier, inc=1, device_id=dev(member(flip, dx, dc)), device_id_type=MESH)
    for k in range(2):
        pl.semaphore_signal(barrier, inc=1, device_id=(dp, (1 - upper) * 2 + k, s), device_id_type=MESH)

    def activation():
        cond = cond_ref[...].astype(jnp.float32)
        return (cond * jax.nn.sigmoid(cond)).astype(jnp.bfloat16)

    def put_rows(row, value, count):
        for t in range(2):
            for i in range(count):
                at = row + t * count + i
                ada_msg[at:at + 1, :] = value[t:t + 1, i * LANES:(i + 1) * LANES]

    def ada_send(other):
        dest = member(*other)
        return pltpu.make_async_remote_copy(ada_msg, ada_in.at[my_head], ada_ss.at[dest], ada_rs.at[my_head], device_id=dev(dest), device_id_type=MESH)

    def ada_recv(other):
        src = member(*other)
        return pltpu.make_async_remote_copy(ada_msg, ada_in.at[src], ada_ss.at[src], ada_rs.at[src], device_id=dev(src), device_id_type=MESH)

    def take_rows(base, layer):
        for t in range(2):
            for tile in range(ada_total):
                part = min(tile // ada_tiles, -(-ada_total // ada_tiles) - 1)
                first = min(ada_tiles * part, ada_total - ada_tiles)
                row = base + t * ada_tiles + tile - first
                cols = slice(tile * LANES, (tile + 1) * LANES)
                mod_s[t * layers + layer:t * layers + layer + 1, cols] = ada_in[part, row:row + 1, :] + bias_s[layer:layer + 1, cols]

    bias_copy.wait()
    bias_s[...] = bias_in[...].astype(jnp.float32)
    head_copy.wait()
    ada_copy.start()
    fa_copy.start()
    k_copy.start()
    v_copy.start()
    head_res = jnp.dot(activation(), head_w[...], preferred_element_type=jnp.float32)
    for t in range(2):
        mod_s[t * layers:t * layers + 1, :2 * width] = head_res[t:t + 1] + bias_s[0:1, :2 * width]
    lat_copy.wait()
    pos_copy.wait()
    pl.semaphore_wait(barrier, members + 1)

    lane2 = lax.broadcasted_iota(jnp.int32, (1, 2 * LANES), 1)
    lane1 = lax.broadcasted_iota(jnp.int32, (1, LANES), 1)
    factor = LOG2_E * head_dim ** -0.5
    tiles = width // LANES
    group_tiles = -(-(blocks * head_dim) // LANES)

    def layer_pass(it, carry):
        t = it // layers
        layer = it % layers
        following = (it + 1) % layers
        more = it + 1 < 2 * layers
        fresh = 1 - t
        bias = lambda lo, hi: bias_s[pl.ds(layer, 1), lo * width:hi * width]
        mod = lambda i: mod_s[pl.ds(it, 1), i * width:(i + 1) * width]

        @pl.when(layer == 0)
        def _():
            emb = lax.dot_general(lat_s[...].astype(jnp.bfloat16), w_in_ref[...], (((0,), (0,)), ((), ())), preferred_element_type=jnp.float32)
            hid_s[...] = (emb + pos_s[...].astype(jnp.float32)).astype(jnp.bfloat16)

        normed = (normalize(hid_s[...].astype(jnp.float32)) * (1.0 + mod(0)) + mod(1)).astype(jnp.bfloat16)
        w_copy(0, layer).wait()

        @pl.when(it == 0)
        def _():
            for which in range(1, 4):
                w_copy(which, 0).start()

        def qkv_send(dest):
            return pltpu.make_async_remote_copy(msg.at[dest], kv.at[fresh, layer, pl.ds(row_own, block_rows), :], qkv_ss.at[dest], qkv_rs.at[my_head], device_id=dev(dest), device_id_type=MESH)

        def qkv_recv(src):
            rows = pl.ds(pl.multiple_of(device_row(src) * patch_rows + src % blocks * block_rows, block_rows), block_rows)
            return pltpu.make_async_remote_copy(msg.at[src], kv.at[fresh, layer, rows, :], qkv_ss.at[src], qkv_rs.at[src], device_id=dev(src), device_id_type=MESH)

        far = 1 - own_group
        wide = group_tiles * LANES
        narrow = width - wide
        far_col = far * narrow
        near_col = (1 - far) * wide
        shift_unit = blocks * head_dim - narrow

        def columns(i, start, size):
            cols = pl.ds(pl.multiple_of(i * width + start, LANES), size)
            bias_cols = pl.ds(pl.multiple_of((6 + i) * width + start, LANES), size)
            part = jnp.dot(normed, qkv_w[:, cols], preferred_element_type=jnp.float32) + bias_s[pl.ds(layer, 1), bias_cols]
            return part.astype(jnp.bfloat16).astype(jnp.float32)

        def pack_group(group, parts):
            parts = [jnp.where(group == 1, pltpu.roll(part, wide - shift_unit, 1), part) for part in parts]

            def window(i, col, place):
                tile = min(col // LANES, group_tiles - 2)
                shift = (place - (col - tile * LANES)) % (2 * LANES)
                part = parts[i][:, tile * LANES:(tile + 2) * LANES]
                return pltpu.roll(part, shift, 1) if shift else part

            for k in range(blocks):
                col = k * head_dim
                block = jnp.where(lane2 < head_dim, window(1, col, 0),
                                  jnp.where(lane2 < 2 * head_dim, window(2, col, head_dim), window(0, col, 2 * head_dim)))
                msg[group * blocks + k] = block.astype(jnp.bfloat16)

        firsts = [columns(i, far_col, wide) for i in range(3)]
        pack_group(far, firsts)
        for dx in far_order:
            for dc in (1, 0):
                qkv_send(far * blocks + column(dx, dc)).start()
        seconds = [columns(i, near_col, narrow) for i in range(3)]
        pack_group(own_group, [jnp.where(far == 0, jnp.concatenate([first[:, narrow:], second], axis=1), jnp.concatenate([second, first[:, :wide - narrow]], axis=1))
                               for first, second in zip(firsts, seconds)])
        for dx in far_order:
            for dc in (1, 0):
                if (dx, dc) != (0, 0):
                    qkv_send(own_group * blocks + column(dx, dc)).start()
        kv[fresh, layer, pl.ds(row_own, block_rows), :] = msg[my_head]

        @pl.when(more)
        def _():
            w_copy(0, following).start()

        @pl.when(it == 0)
        def _():
            act = activation()
            ada_copy.wait()
            for part_layer in range(layers):
                put_rows(part_layer * 2 * ada_tiles, jnp.dot(act, ada_w[part_layer], preferred_element_type=jnp.float32), ada_tiles)
            fa_copy.wait()
            put_rows(layers * 2 * ada_tiles, jnp.dot(act, fa_w[...], preferred_element_type=jnp.float32), fa_tiles)
            for other in others:
                ada_send(other).start()
            ada_in[my_head] = ada_msg[...]
            k_copy.wait()
            v_copy.wait()

        @pl.when(t == 0)
        def _():
            for kp in range(1, chips_y):
                @pl.when(kp > 2 * upper)
                def _():
                    rows = slice(kp * patch_rows, (kp + 1) * patch_rows)
                    stack = jnp.concatenate([old_s[0, layer, :, rows].astype(jnp.float32), old_s[1, layer, :, rows].astype(jnp.float32),
                                             jnp.zeros((2 * LANES - 2 * head_dim, patch_rows), jnp.float32)], axis=0)
                    kv[0, layer, rows, :] = stack.T.astype(jnp.bfloat16)

        for other in others:
            qkv_recv(member(*other)).wait_recv()

        def half_copy(half):
            rows = pl.ds(pl.multiple_of(half * half_rows, half_rows), half_rows)
            return pltpu.make_async_remote_copy(kv.at[fresh, layer, rows, :], kv.at[fresh, layer, rows, :], fwd_ss.at[layer], fwd_rs.at[layer], device_id=partner, device_id_type=MESH)

        def stored_copy():
            rows = pl.ds(half_rows, half_rows)
            return pltpu.make_async_remote_copy(kv.at[1, layer, rows, :], kv.at[1, layer, rows, :], fwd_ss.at[layer], fwd_rs.at[layer], device_id=partner, device_id_type=MESH)

        @pl.when(jnp.logical_and(upper == 0, t == 1))
        def _():
            stored_copy().wait_recv()

        @pl.when(upper == 0)
        def _():
            half_copy(0).start()

        @pl.when(upper == 1)
        def _():
            half_copy(0).wait_recv()

        def o_send(p, col):
            rows = pl.ds(pl.multiple_of((p % 2) * patch_rows + col * block_rows, block_rows), block_rows)
            dest = jnp.where(p == y, own_group, 1 - own_group) * blocks + col
            return pltpu.make_async_remote_copy(o_msg.at[rows, :], o_in.at[my_head], o_ss.at[dest], o_rs.at[my_head], device_id=(dp, p, col), device_id_type=MESH)

        def o_recv(src):
            return pltpu.make_async_remote_copy(o_msg.at[pl.ds(0, block_rows), :], o_in.at[src], o_ss.at[src], o_rs.at[src], device_id=dev(src), device_id_type=MESH)

        pair = 2 * block_rows

        def queries(flip, dxs):
            p = 2 * upper + (lane_row + flip) % 2
            offsets = [(x + dx) % chips_x * pair for dx in dxs]
            if len(dxs) == chips_x:
                q_part = kv[fresh, layer, pl.ds(pl.multiple_of(p * patch_rows, patch_rows), patch_rows), LANES:]
            else:
                q_part = jnp.concatenate([kv[fresh, layer, pl.ds(pl.multiple_of(p * patch_rows + at, pair), pair), LANES:] for at in offsets], axis=0)
            q_part = pltpu.roll(q_part.astype(jnp.float32), 2 * LANES - 2 * head_dim, 1)
            return jnp.where(lane1 < head_dim, q_part, 0.0).astype(jnp.bfloat16)

        def blocks_of(flip, lanes):
            p = 2 * upper + (lane_row + flip) % 2
            return [kv[jnp.where(kp <= p, fresh, 1 - fresh), layer, kp * patch_rows:(kp + 1) * patch_rows, :lanes] for kp in range(chips_y)]

        def score(flip, dxs):
            q_part = queries(flip, dxs)
            return [lax.dot_general(q_part, block, (((1,), (1,)), ((), ())), preferred_element_type=jnp.float32) for block in blocks_of(flip, LANES)]

        def probs(scores):
            scores = jnp.concatenate(scores, axis=1)
            top = jnp.max(scores, axis=-1, keepdims=True)
            e = jnp.exp2((scores - top) * factor)
            return (e * (1.0 / jnp.sum(e, axis=-1, keepdims=True))).astype(jnp.bfloat16)

        def values(flip, dxs, prob):
            p = 2 * upper + (lane_row + flip) % 2
            o = None
            for kp, block in enumerate(blocks_of(flip, 2 * LANES)):
                term = jnp.dot(prob[:, kp * patch_rows:(kp + 1) * patch_rows], block, preferred_element_type=jnp.float32)
                o = term if o is None else o + term
            o = pltpu.roll(o, 2 * LANES - head_dim, 1)[:, :LANES].astype(jnp.bfloat16)
            if len(dxs) == chips_x:
                o_msg[pl.ds(pl.multiple_of((p % 2) * patch_rows, patch_rows), patch_rows), :] = o
            else:
                for i, dx in enumerate(dxs):
                    o_msg[pl.ds(pl.multiple_of((p % 2) * patch_rows + (x + dx) % chips_x * pair, pair), pair), :] = o[i * pair:(i + 1) * pair]

        def send_rows(flip, dxs):
            p = 2 * upper + (lane_row + flip) % 2
            for dx in dxs:
                for dc in (1, 0):
                    if (flip, dx, dc) != (0, 0, 0):
                        o_send(p, column(dx, dc)).start()

        chunks = [(flip, far_order) for flip in (1, 0)]
        all_scores = [score(*chunk) for chunk in chunks]
        all_probs = [probs(scores) for scores in all_scores]
        for (flip, dxs), prob in zip(chunks, all_probs):
            values(flip, dxs, prob)
        for flip, dxs in chunks:
            send_rows(flip, dxs)

        o_in[my_head] = o_msg[pl.ds(pl.multiple_of(lane_row * patch_rows + s * block_rows, block_rows), block_rows), :]

        @pl.when(jnp.logical_and(upper == 1, t == 0))
        def _():
            half_copy(1).start()

        @pl.when(it == 0)
        def _():
            for other in others:
                ada_recv(other).wait_recv()
            for late in range(layers):
                take_rows(late * 2 * ada_tiles, late)
            for step in range(2):
                for tile in range(fa_total):
                    row = layers * 2 * ada_tiles + step * fa_tiles + tile % fa_tiles
                    cols = slice(tile * LANES, (tile + 1) * LANES)
                    fmod_s[step:step + 1, cols] = ada_in[tile // fa_tiles, row:row + 1, :] + b_fa_ref[cols].astype(jnp.float32).reshape(1, LANES)
            for other in others:
                ada_send(other).wait_send()

        for other in others:
            o_recv(member(*other)).wait_recv()

        pieces = [None] * tiles
        for head in range(heads):
            at = head * head_dim
            tile, off = at // LANES, at % LANES
            part = o_in[head].astype(jnp.float32)
            if off:
                part = pltpu.roll(part, off, 1)
            pieces[tile] = part if pieces[tile] is None else jnp.where(lane1 >= off, part, pieces[tile])
            if off + head_dim > LANES:
                pieces[tile + 1] = part
        attn = jnp.concatenate(pieces, axis=1).astype(jnp.bfloat16)
        w_copy(1, layer).wait()
        proj = jnp.dot(attn, o_w[...], preferred_element_type=jnp.float32) + bias(9, 10)

        @pl.when(more)
        def _():
            w_copy(1, following).start()

        residual = hid_s[...].astype(jnp.float32) + mod(2) * proj
        mlp_in = (normalize(residual) * (1.0 + mod(3)) + mod(4)).astype(jnp.bfloat16)
        w_copy(2, layer).wait()
        up_cols = up_w.shape[1] // 4
        w_copy(3, layer).wait()
        down = bias(14, 15)
        for i in range(4):
            cols = slice(i * up_cols, (i + 1) * up_cols)
            up_bias = bias_s[pl.ds(layer, 1), 10 * width + i * up_cols:10 * width + (i + 1) * up_cols]
            up = jnp.dot(mlp_in, up_w[:, cols], preferred_element_type=jnp.float32) + up_bias
            mid = jax.nn.gelu(up, approximate=True).astype(jnp.bfloat16)
            down = down + jnp.dot(mid, down_w[cols, :], preferred_element_type=jnp.float32)

        @pl.when(more)
        def _():
            w_copy(2, following).start()

        hid_s[...] = (residual + mod(5) * down).astype(jnp.bfloat16)

        @pl.when(more)
        def _():
            w_copy(3, following).start()

        @pl.when(layer == layers - 1)
        def _():
            scale_out = fmod_s[pl.ds(t, 1), :width]
            shift_out = fmod_s[pl.ds(t, 1), width:]
            out_rows = (normalize(hid_s[...].astype(jnp.float32)) * (1.0 + scale_out) + shift_out).astype(jnp.bfloat16)
            velocity = lax.dot_general(w_out_ref[...], out_rows, (((1,), (1,)), ((), ())), preferred_element_type=jnp.float32)
            lat_s[...] = lat_s[...] + step_ref[t] * velocity

        for other in others:
            qkv_send(member(*other)).wait_send()
            flip, dx, dc = other
            o_send(2 * upper + (lane_row + flip) % 2, column(dx, dc)).wait_send()

        @pl.when(upper == 0)
        def _():
            half_copy(0).wait_send()

        @pl.when(jnp.logical_and(upper == 1, t == 0))
        def _():
            half_copy(1).wait_send()

        return carry

    lax.fori_loop(0, 2 * layers, layer_pass, 0)

    def out_copy(k, src_side):
        row = (y + k) % chips_y
        slot = row if src_side else y
        return pltpu.make_async_remote_copy(lat_s, out_ref.at[slot], out_ss.at[row], out_rs.at[slot], device_id=(dp, row, s), device_id_type=MESH)

    for k in range(1, chips_y):
        out_copy(k, False).start()
    own_copy = pltpu.make_async_copy(lat_s, out_ref.at[y], load_sem.at[0])
    own_copy.start()
    for k in range(1, chips_y):
        out_copy(k, True).wait_recv()
    own_copy.wait()
    for k in range(1, chips_y):
        out_copy(k, False).wait_send()


def solution(mesh):
    chips_y = mesh.shape["pp"]
    chips_x = mesh.shape["sp"] // 2
    row_spec = P("dp", "sp", None)
    full_spec = P()
    buf_spec = P("dp", None, None, None)
    in_specs = (row_spec, P(None, "sp", None), P("dp", None), P("dp"), full_spec, full_spec, full_spec, full_spec, full_spec, full_spec, full_spec, full_spec, full_spec, full_spec, buf_spec, buf_spec)

    def device_fn(latent_in, pos_embed, condition, step_size, w_in, w_ada, w_qkv, w_o, w_up, w_down, b_layer, w_fa, b_fa, w_out, k_old, v_old):
        patches, block_rows, latent_dim = latent_in.shape
        layers, width = w_qkv.shape[:2]
        tokens, heads, head_dim = k_old.shape[1:]
        members = 4 * chips_x
        ada_tiles = -(-(w_ada.shape[2] // LANES) // members)
        fa_tiles = -(-(w_fa.shape[1] // LANES) // members)
        ada_rows = 2 * (layers * ada_tiles + fa_tiles)
        half_rows = 2 * block_rows * 2 * chips_x
        dims = (chips_x, chips_y, layers, block_rows, width, heads, head_dim)
        bf16, f32 = jnp.bfloat16, jnp.float32
        vmem = pl.BlockSpec(memory_space=pltpu.VMEM)
        hbm = pl.BlockSpec(memory_space=pl.ANY)
        dma = pltpu.SemaphoreType.DMA
        latent_t = jnp.transpose(latent_in, (0, 2, 1))
        k_t = jnp.transpose(k_old, (0, 2, 3, 1))
        v_t = jnp.transpose(v_old, (0, 2, 3, 1))
        result = pl.pallas_call(
            functools.partial(kernel, dims),
            out_shape=jax.ShapeDtypeStruct(latent_t.shape, f32),
            in_specs=[vmem, pl.BlockSpec(memory_space=pltpu.SMEM), vmem, vmem, vmem] + [hbm] * 11,
            out_specs=hbm,
            scratch_shapes=[
                pltpu.VMEM((width, 2 * width), bf16),
                pltpu.VMEM((layers, width, ada_tiles * LANES), bf16),
                pltpu.VMEM((width, fa_tiles * LANES), bf16),
                pltpu.VMEM(w_qkv.shape[1:], bf16),
                pltpu.VMEM(w_o.shape[1:], bf16),
                pltpu.VMEM(w_up.shape[1:], bf16),
                pltpu.VMEM(w_down.shape[1:], bf16),
                pltpu.VMEM((2, layers, tokens, 2 * LANES), bf16),
                pltpu.VMEM((2, layers, head_dim, tokens), bf16),
                pltpu.VMEM((members, block_rows, 2 * LANES), bf16),
                pltpu.VMEM((half_rows, LANES), bf16),
                pltpu.VMEM((members, block_rows, LANES), bf16),
                pltpu.VMEM((ada_rows, LANES), f32),
                pltpu.VMEM((members, ada_rows, LANES), f32),
                pltpu.VMEM((2 * layers, w_ada.shape[2]), f32),
                pltpu.VMEM((2, w_fa.shape[1]), f32),
                pltpu.VMEM(b_layer.shape, bf16),
                pltpu.VMEM(b_layer.shape, f32),
                pltpu.VMEM((block_rows, width), bf16),
                pltpu.VMEM((latent_dim, block_rows), f32),
                pltpu.VMEM((block_rows, width), bf16),
                dma((4,)), dma((8,)), dma((members,)), dma((members,)), dma((members,)), dma((members,)), dma((members,)), dma((members,)),
                dma((layers,)), dma((layers,)), dma((chips_y,)), dma((chips_y,)),
            ],
            compiler_params=pltpu.CompilerParams(collective_id=0, has_side_effects=True, vmem_limit_bytes=60 * 1024 * 1024),
        )(condition, step_size, w_in, b_fa, w_out.T, latent_t, pos_embed, b_layer, k_t, v_t, w_ada, w_fa, w_qkv, w_o, w_up, w_down)
        return jnp.transpose(result, (0, 2, 1))

    return jax.shard_map(device_fn, mesh=mesh, in_specs=in_specs, out_specs=row_spec, check_vma=False)
```

```python
import functools

import jax
import jax.numpy as jnp
from jax import lax
from jax.experimental import pallas as pl
from jax.experimental.pallas import tpu as pltpu
from jax.sharding import PartitionSpec as P

LN_EPS = 1e-6
LANES = 128
LOG2_E = 1.4426950408889634
MESH = pl.DeviceIdType.MESH


def normalize(hidden):
    mean_val = jnp.mean(hidden, axis=-1, keepdims=True)
    centered = hidden - mean_val
    var_val = jnp.mean(centered * centered, axis=-1, keepdims=True)
    return centered * lax.rsqrt(var_val + LN_EPS)


def kernel(dims, cond_ref, step_ref, w_in_ref, b_fa_ref, w_out_ref,
           latent_hbm, pos_hbm, b_layer_hbm, k_hbm, v_hbm, w_ada_hbm, w_fa_hbm, w_qkv_hbm, w_o_hbm, w_up_hbm, w_down_hbm,
           out_ref,
           head_w, ada_w, fa_w, qkv_w, o_w, up_w, down_w, kv, old_s, msg, o_msg, o_in, ada_msg, ada_in,
           mod_s, fmod_s, bias_in, bias_s, hid_s, lat_s, pos_s, pack_out, pack_in,
           w_sem, load_sem, ada_ss, ada_rs, qkv_ss, qkv_rs, o_ss, o_rs, fwd_ss, fwd_rs, out_ss, out_rs, pack_ss, pack_rs):
    (chips_x, chips_y, layers, block_rows, width, heads, head_dim) = dims
    blocks = 2 * chips_x
    patch_rows = block_rows * blocks
    half_rows = 2 * patch_rows
    members = 2 * blocks
    far_order = sorted(range(chips_x), key=lambda d: -min(d, chips_x - d))
    dp = lax.axis_index("dp")
    y = lax.axis_index("pp")
    s = lax.axis_index("sp")
    x = s // 2
    core = s % 2
    upper = y // 2
    lane_row = y % 2
    own_group = jnp.where(upper == 0, lane_row, 1 - lane_row)
    my_head = own_group * blocks + s
    row_own = pl.multiple_of(y * patch_rows + s * block_rows, block_rows)

    def group_row(group):
        return jnp.where(upper == 0, group, chips_y - 1 - group)

    def column(dx, dc):
        return 2 * ((x + dx) % chips_x) + (core + dc) % 2

    def device_row(head):
        return group_row(head // blocks)

    def dev(head):
        return (dp, device_row(head), head % blocks)

    others = [(flip, dx, dc) for flip in (1, 0) for dx in far_order for dc in (1, 0) if (flip, dx, dc) != (0, 0, 0)]

    def member(flip, dx, dc):
        return (own_group + flip) % 2 * blocks + column(dx, dc)

    partner = (dp, chips_y - 1 - y, s)

    ada_tiles = ada_w.shape[2] // LANES
    ada_total = w_ada_hbm.shape[2] // LANES
    fa_tiles = fa_w.shape[1] // LANES
    fa_total = w_fa_hbm.shape[1] // LANES

    ada_col = pl.multiple_of(jnp.minimum(ada_tiles * my_head, ada_total - ada_tiles) * LANES, LANES)
    fa_col = pl.multiple_of(jnp.minimum(fa_tiles * my_head, fa_total - fa_tiles) * LANES, LANES)
    head_copy = pltpu.make_async_copy(w_ada_hbm.at[0, :, pl.ds(0, head_w.shape[1])], head_w, load_sem.at[0])
    head_copy.start()
    bias_copy = pltpu.make_async_copy(b_layer_hbm, bias_in, load_sem.at[2])
    bias_copy.start()
    pos_copy = pltpu.make_async_copy(pos_hbm.at[y], pos_s, load_sem.at[3])
    pos_copy.start()
    lat_copy = pltpu.make_async_copy(latent_hbm.at[y], lat_s, load_sem.at[7])
    lat_copy.start()
    ada_copy = pltpu.make_async_copy(w_ada_hbm.at[:, :, pl.ds(ada_col, ada_w.shape[2])], ada_w, load_sem.at[6])
    fa_copy = pltpu.make_async_copy(w_fa_hbm.at[:, pl.ds(fa_col, fa_w.shape[1])], fa_w, load_sem.at[1])
    k_copy = pltpu.make_async_copy(k_hbm.at[:, my_head], old_s.at[0], load_sem.at[4])
    v_copy = pltpu.make_async_copy(v_hbm.at[:, my_head], old_s.at[1], load_sem.at[5])

    def w_copy(which, layer):
        src, dst = ((w_qkv_hbm, qkv_w), (w_o_hbm, o_w), (w_up_hbm, up_w), (w_down_hbm, down_w))[which]
        return pltpu.make_async_copy(src.at[layer], dst, w_sem.at[which])

    w_copy(0, 0).start()

    barrier = pltpu.get_barrier_semaphore()
    for flip, dx, dc in others:
        pl.semaphore_signal(barrier, inc=1, device_id=dev(member(flip, dx, dc)), device_id_type=MESH)
    for k in range(2):
        pl.semaphore_signal(barrier, inc=1, device_id=(dp, (1 - upper) * 2 + k, s), device_id_type=MESH)

    def activation():
        cond = cond_ref[...].astype(jnp.float32)
        return (cond * jax.nn.sigmoid(cond)).astype(jnp.bfloat16)

    def put_rows(row, value, count):
        for t in range(2):
            for i in range(count):
                at = row + t * count + i
                ada_msg[at:at + 1, :] = value[t:t + 1, i * LANES:(i + 1) * LANES]

    def ada_send(other):
        dest = member(*other)
        return pltpu.make_async_remote_copy(ada_msg, ada_in.at[my_head], ada_ss.at[dest], ada_rs.at[my_head], device_id=dev(dest), device_id_type=MESH)

    def ada_recv(other):
        src = member(*other)
        return pltpu.make_async_remote_copy(ada_msg, ada_in.at[src], ada_ss.at[src], ada_rs.at[src], device_id=dev(src), device_id_type=MESH)

    def take_rows(base, layer):
        for t in range(2):
            for tile in range(ada_total):
                part = min(tile // ada_tiles, -(-ada_total // ada_tiles) - 1)
                first = min(ada_tiles * part, ada_total - ada_tiles)
                row = base + t * ada_tiles + tile - first
                cols = slice(tile * LANES, (tile + 1) * LANES)
                mod_s[t * layers + layer:t * layers + layer + 1, cols] = ada_in[part, row:row + 1, :] + bias_s[layer:layer + 1, cols]

    bias_copy.wait()
    bias_s[...] = bias_in[...].astype(jnp.float32)
    head_copy.wait()
    ada_copy.start()
    fa_copy.start()
    k_copy.start()
    v_copy.start()
    head_res = jnp.dot(activation(), head_w[...], preferred_element_type=jnp.float32)
    for t in range(2):
        mod_s[t * layers:t * layers + 1, :2 * width] = head_res[t:t + 1] + bias_s[0:1, :2 * width]
    lat_copy.wait()
    pos_copy.wait()
    pl.semaphore_wait(barrier, members + 1)

    lane2 = lax.broadcasted_iota(jnp.int32, (1, 2 * LANES), 1)
    lane1 = lax.broadcasted_iota(jnp.int32, (1, LANES), 1)
    factor = LOG2_E * head_dim ** -0.5
    tiles = width // LANES
    group_tiles = -(-(blocks * head_dim) // LANES)
    rest = 2 * head_dim - LANES
    packs = LANES // rest
    pack_rows = half_rows // packs

    def layer_pass(it, carry):
        t = it // layers
        layer = it % layers
        following = (it + 1) % layers
        more = it + 1 < 2 * layers
        fresh = 1 - t
        bias = lambda lo, hi: bias_s[pl.ds(layer, 1), lo * width:hi * width]
        mod = lambda i: mod_s[pl.ds(it, 1), i * width:(i + 1) * width]

        @pl.when(layer == 0)
        def _():
            emb = lax.dot_general(lat_s[...].astype(jnp.bfloat16), w_in_ref[...], (((0,), (0,)), ((), ())), preferred_element_type=jnp.float32)
            hid_s[...] = (emb + pos_s[...].astype(jnp.float32)).astype(jnp.bfloat16)

        normed = (normalize(hid_s[...].astype(jnp.float32)) * (1.0 + mod(0)) + mod(1)).astype(jnp.bfloat16)
        w_copy(0, layer).wait()

        @pl.when(it == 0)
        def _():
            for which in range(1, 4):
                w_copy(which, 0).start()

        def qkv_send(dest):
            return pltpu.make_async_remote_copy(msg.at[dest], kv.at[fresh, layer, pl.ds(row_own, block_rows), :], qkv_ss.at[dest], qkv_rs.at[my_head], device_id=dev(dest), device_id_type=MESH)

        def qkv_recv(src):
            rows = pl.ds(pl.multiple_of(device_row(src) * patch_rows + src % blocks * block_rows, block_rows), block_rows)
            return pltpu.make_async_remote_copy(msg.at[src], kv.at[fresh, layer, rows, :], qkv_ss.at[src], qkv_rs.at[src], device_id=dev(src), device_id_type=MESH)

        far = 1 - own_group
        wide = group_tiles * LANES
        narrow = width - wide
        far_col = far * narrow
        near_col = (1 - far) * wide
        shift_unit = blocks * head_dim - narrow

        def columns(i, start, size):
            cols = pl.ds(pl.multiple_of(i * width + start, LANES), size)
            bias_cols = pl.ds(pl.multiple_of((6 + i) * width + start, LANES), size)
            part = jnp.dot(normed, qkv_w[:, cols], preferred_element_type=jnp.float32) + bias_s[pl.ds(layer, 1), bias_cols]
            return part.astype(jnp.bfloat16).astype(jnp.float32)

        def pack_group(group, parts):
            parts = [jnp.where(group == 1, pltpu.roll(part, wide - shift_unit, 1), part) for part in parts]

            def window(i, col, place):
                tile = min(col // LANES, group_tiles - 2)
                shift = (place - (col - tile * LANES)) % (2 * LANES)
                part = parts[i][:, tile * LANES:(tile + 2) * LANES]
                return pltpu.roll(part, shift, 1) if shift else part

            for k in range(blocks):
                col = k * head_dim
                block = jnp.where(lane2 < head_dim, window(1, col, 0),
                                  jnp.where(lane2 < 2 * head_dim, window(2, col, head_dim), window(0, col, 2 * head_dim)))
                msg[group * blocks + k] = block.astype(jnp.bfloat16)

        firsts = [columns(i, far_col, wide) for i in range(3)]
        pack_group(far, firsts)
        for dx in far_order:
            for dc in (1, 0):
                qkv_send(far * blocks + column(dx, dc)).start()
        seconds = [columns(i, near_col, narrow) for i in range(3)]
        pack_group(own_group, [jnp.where(far == 0, jnp.concatenate([first[:, narrow:], second], axis=1), jnp.concatenate([second, first[:, :wide - narrow]], axis=1))
                               for first, second in zip(firsts, seconds)])
        for dx in far_order:
            for dc in (1, 0):
                if (dx, dc) != (0, 0):
                    qkv_send(own_group * blocks + column(dx, dc)).start()
        kv[fresh, layer, pl.ds(row_own, block_rows), :] = msg[my_head]

        @pl.when(more)
        def _():
            w_copy(0, following).start()

        @pl.when(it == 0)
        def _():
            act = activation()
            ada_copy.wait()
            for part_layer in range(layers):
                put_rows(part_layer * 2 * ada_tiles, jnp.dot(act, ada_w[part_layer], preferred_element_type=jnp.float32), ada_tiles)
            fa_copy.wait()
            put_rows(layers * 2 * ada_tiles, jnp.dot(act, fa_w[...], preferred_element_type=jnp.float32), fa_tiles)
            for other in others:
                ada_send(other).start()
            ada_in[my_head] = ada_msg[...]
            k_copy.wait()
            v_copy.wait()

        @pl.when(t == 0)
        def _():
            for kp in range(1, chips_y):
                @pl.when(kp > 2 * upper)
                def _():
                    rows = slice(kp * patch_rows, (kp + 1) * patch_rows)
                    stack = jnp.concatenate([old_s[0, layer, :, rows].astype(jnp.float32), old_s[1, layer, :, rows].astype(jnp.float32),
                                             jnp.zeros((2 * LANES - 2 * head_dim, patch_rows), jnp.float32)], axis=0)
                    kv[0, layer, rows, :] = stack.T.astype(jnp.bfloat16)

        for other in others:
            qkv_recv(member(*other)).wait_recv()

        def lower_copies():
            rows = pl.ds(0, half_rows)
            return (pltpu.make_async_remote_copy(kv.at[fresh, layer, rows, pl.ds(0, LANES)], kv.at[fresh, layer, rows, pl.ds(0, LANES)], fwd_ss.at[layer], fwd_rs.at[layer], device_id=partner, device_id_type=MESH),
                    pltpu.make_async_remote_copy(pack_out, pack_in.at[layer], pack_ss.at[layer], pack_rs.at[layer], device_id=partner, device_id_type=MESH))

        def stored_copy():
            rows = pl.ds(half_rows, half_rows)
            return pltpu.make_async_remote_copy(kv.at[1, layer, rows, :], kv.at[1, layer, rows, :], fwd_ss.at[layer], fwd_rs.at[layer], device_id=partner, device_id_type=MESH)

        @pl.when(jnp.logical_and(upper == 0, t == 1))
        def _():
            stored_copy().wait_recv()

        @pl.when(upper == 0)
        def _():
            packed = None
            for r in range(packs):
                part = kv[fresh, layer, r * pack_rows:(r + 1) * pack_rows, LANES:].astype(jnp.float32)
                if r:
                    part = pltpu.roll(part, r * rest, 1)
                packed = part if packed is None else jnp.where(lane1 >= r * rest, part, packed)
            pack_out[...] = packed.astype(jnp.bfloat16)
            for copy in lower_copies():
                copy.start()

        @pl.when(upper == 1)
        def _():
            for copy in lower_copies():
                copy.wait_recv()
            packed = pack_in[layer].astype(jnp.float32)
            for r in range(packs):
                part = pltpu.roll(packed, LANES - r * rest, 1) if r else packed
                kv[fresh, layer, r * pack_rows:(r + 1) * pack_rows, LANES:] = part.astype(jnp.bfloat16)

        def o_send(p, col):
            rows = pl.ds(pl.multiple_of((p % 2) * patch_rows + col * block_rows, block_rows), block_rows)
            dest = jnp.where(p == y, own_group, 1 - own_group) * blocks + col
            return pltpu.make_async_remote_copy(o_msg.at[rows, :], o_in.at[my_head], o_ss.at[dest], o_rs.at[my_head], device_id=(dp, p, col), device_id_type=MESH)

        def o_recv(src):
            return pltpu.make_async_remote_copy(o_msg.at[pl.ds(0, block_rows), :], o_in.at[src], o_ss.at[src], o_rs.at[src], device_id=dev(src), device_id_type=MESH)

        pair = 2 * block_rows

        def queries(flip, dxs):
            p = 2 * upper + (lane_row + flip) % 2
            offsets = [(x + dx) % chips_x * pair for dx in dxs]
            if len(dxs) == chips_x:
                q_part = kv[fresh, layer, pl.ds(pl.multiple_of(p * patch_rows, patch_rows), patch_rows), LANES:]
            else:
                q_part = jnp.concatenate([kv[fresh, layer, pl.ds(pl.multiple_of(p * patch_rows + at, pair), pair), LANES:] for at in offsets], axis=0)
            q_part = pltpu.roll(q_part.astype(jnp.float32), 2 * LANES - 2 * head_dim, 1)
            return jnp.where(lane1 < head_dim, q_part, 0.0).astype(jnp.bfloat16)

        def blocks_of(flip, lanes):
            p = 2 * upper + (lane_row + flip) % 2
            return [kv[jnp.where(kp <= p, fresh, 1 - fresh), layer, kp * patch_rows:(kp + 1) * patch_rows, :lanes] for kp in range(chips_y)]

        def score(flip, dxs):
            q_part = queries(flip, dxs)
            return [lax.dot_general(q_part, block, (((1,), (1,)), ((), ())), preferred_element_type=jnp.float32) for block in blocks_of(flip, LANES)]

        def probs(scores):
            scores = jnp.concatenate(scores, axis=1)
            top = jnp.max(scores, axis=-1, keepdims=True)
            e = jnp.exp2((scores - top) * factor)
            return (e * (1.0 / jnp.sum(e, axis=-1, keepdims=True))).astype(jnp.bfloat16)

        def values(flip, dxs, prob):
            p = 2 * upper + (lane_row + flip) % 2
            o = None
            for kp, block in enumerate(blocks_of(flip, 2 * LANES)):
                term = jnp.dot(prob[:, kp * patch_rows:(kp + 1) * patch_rows], block, preferred_element_type=jnp.float32)
                o = term if o is None else o + term
            o = pltpu.roll(o, 2 * LANES - head_dim, 1)[:, :LANES].astype(jnp.bfloat16)
            if len(dxs) == chips_x:
                o_msg[pl.ds(pl.multiple_of((p % 2) * patch_rows, patch_rows), patch_rows), :] = o
            else:
                for i, dx in enumerate(dxs):
                    o_msg[pl.ds(pl.multiple_of((p % 2) * patch_rows + (x + dx) % chips_x * pair, pair), pair), :] = o[i * pair:(i + 1) * pair]

        def send_rows(flip, dxs):
            p = 2 * upper + (lane_row + flip) % 2
            for dx in dxs:
                for dc in (1, 0):
                    if (flip, dx, dc) != (0, 0, 0):
                        o_send(p, column(dx, dc)).start()

        chunks = [(flip, far_order) for flip in (1, 0)]
        all_scores = [score(*chunk) for chunk in chunks]
        all_probs = [probs(scores) for scores in all_scores]
        for (flip, dxs), prob in zip(chunks, all_probs):
            values(flip, dxs, prob)
        for flip, dxs in chunks:
            send_rows(flip, dxs)

        o_in[my_head] = o_msg[pl.ds(pl.multiple_of(lane_row * patch_rows + s * block_rows, block_rows), block_rows), :]

        @pl.when(jnp.logical_and(upper == 1, t == 0))
        def _():
            stored_copy().start()

        @pl.when(it == 0)
        def _():
            for other in others:
                ada_recv(other).wait_recv()
            for late in range(layers):
                take_rows(late * 2 * ada_tiles, late)
            for step in range(2):
                for tile in range(fa_total):
                    row = layers * 2 * ada_tiles + step * fa_tiles + tile % fa_tiles
                    cols = slice(tile * LANES, (tile + 1) * LANES)
                    fmod_s[step:step + 1, cols] = ada_in[tile // fa_tiles, row:row + 1, :] + b_fa_ref[cols].astype(jnp.float32).reshape(1, LANES)
            for other in others:
                ada_send(other).wait_send()

        for other in others:
            o_recv(member(*other)).wait_recv()

        pieces = [None] * tiles
        for head in range(heads):
            at = head * head_dim
            tile, off = at // LANES, at % LANES
            part = o_in[head].astype(jnp.float32)
            if off:
                part = pltpu.roll(part, off, 1)
            pieces[tile] = part if pieces[tile] is None else jnp.where(lane1 >= off, part, pieces[tile])
            if off + head_dim > LANES:
                pieces[tile + 1] = part
        attn = jnp.concatenate(pieces, axis=1).astype(jnp.bfloat16)
        w_copy(1, layer).wait()
        proj = jnp.dot(attn, o_w[...], preferred_element_type=jnp.float32) + bias(9, 10)

        @pl.when(more)
        def _():
            w_copy(1, following).start()

        residual = hid_s[...].astype(jnp.float32) + mod(2) * proj
        mlp_in = (normalize(residual) * (1.0 + mod(3)) + mod(4)).astype(jnp.bfloat16)
        w_copy(2, layer).wait()
        up_cols = up_w.shape[1] // 4
        w_copy(3, layer).wait()
        down = bias(14, 15)
        for i in range(4):
            cols = slice(i * up_cols, (i + 1) * up_cols)
            up_bias = bias_s[pl.ds(layer, 1), 10 * width + i * up_cols:10 * width + (i + 1) * up_cols]
            up = jnp.dot(mlp_in, up_w[:, cols], preferred_element_type=jnp.float32) + up_bias
            mid = jax.nn.gelu(up, approximate=True).astype(jnp.bfloat16)
            down = down + jnp.dot(mid, down_w[cols, :], preferred_element_type=jnp.float32)

        @pl.when(more)
        def _():
            w_copy(2, following).start()

        hid_s[...] = (residual + mod(5) * down).astype(jnp.bfloat16)

        @pl.when(more)
        def _():
            w_copy(3, following).start()

        @pl.when(layer == layers - 1)
        def _():
            scale_out = fmod_s[pl.ds(t, 1), :width]
            shift_out = fmod_s[pl.ds(t, 1), width:]
            out_rows = (normalize(hid_s[...].astype(jnp.float32)) * (1.0 + scale_out) + shift_out).astype(jnp.bfloat16)
            velocity = lax.dot_general(w_out_ref[...], out_rows, (((1,), (1,)), ((), ())), preferred_element_type=jnp.float32)
            lat_s[...] = lat_s[...] + step_ref[t] * velocity

        for other in others:
            qkv_send(member(*other)).wait_send()
            flip, dx, dc = other
            o_send(2 * upper + (lane_row + flip) % 2, column(dx, dc)).wait_send()

        @pl.when(upper == 0)
        def _():
            for copy in lower_copies():
                copy.wait_send()

        @pl.when(jnp.logical_and(upper == 1, t == 0))
        def _():
            stored_copy().wait_send()

        return carry

    lax.fori_loop(0, 2 * layers, layer_pass, 0)

    def out_copy(k, src_side):
        row = (y + k) % chips_y
        slot = row if src_side else y
        return pltpu.make_async_remote_copy(lat_s, out_ref.at[slot], out_ss.at[row], out_rs.at[slot], device_id=(dp, row, s), device_id_type=MESH)

    for k in range(1, chips_y):
        out_copy(k, False).start()
    own_copy = pltpu.make_async_copy(lat_s, out_ref.at[y], load_sem.at[0])
    own_copy.start()
    for k in range(1, chips_y):
        out_copy(k, True).wait_recv()
    own_copy.wait()
    for k in range(1, chips_y):
        out_copy(k, False).wait_send()


def solution(mesh):
    chips_y = mesh.shape["pp"]
    chips_x = mesh.shape["sp"] // 2
    row_spec = P("dp", "sp", None)
    full_spec = P()
    buf_spec = P("dp", None, None, None)
    in_specs = (row_spec, P(None, "sp", None), P("dp", None), P("dp"), full_spec, full_spec, full_spec, full_spec, full_spec, full_spec, full_spec, full_spec, full_spec, full_spec, buf_spec, buf_spec)

    def device_fn(latent_in, pos_embed, condition, step_size, w_in, w_ada, w_qkv, w_o, w_up, w_down, b_layer, w_fa, b_fa, w_out, k_old, v_old):
        patches, block_rows, latent_dim = latent_in.shape
        layers, width = w_qkv.shape[:2]
        tokens, heads, head_dim = k_old.shape[1:]
        members = 4 * chips_x
        ada_tiles = -(-(w_ada.shape[2] // LANES) // members)
        fa_tiles = -(-(w_fa.shape[1] // LANES) // members)
        ada_rows = 2 * (layers * ada_tiles + fa_tiles)
        half_rows = 2 * block_rows * 2 * chips_x
        dims = (chips_x, chips_y, layers, block_rows, width, heads, head_dim)
        bf16, f32 = jnp.bfloat16, jnp.float32
        vmem = pl.BlockSpec(memory_space=pltpu.VMEM)
        hbm = pl.BlockSpec(memory_space=pl.ANY)
        dma = pltpu.SemaphoreType.DMA
        latent_t = jnp.transpose(latent_in, (0, 2, 1))
        k_t = jnp.transpose(k_old, (0, 2, 3, 1))
        v_t = jnp.transpose(v_old, (0, 2, 3, 1))
        result = pl.pallas_call(
            functools.partial(kernel, dims),
            out_shape=jax.ShapeDtypeStruct(latent_t.shape, f32),
            in_specs=[vmem, pl.BlockSpec(memory_space=pltpu.SMEM), vmem, vmem, vmem] + [hbm] * 11,
            out_specs=hbm,
            scratch_shapes=[
                pltpu.VMEM((width, 2 * width), bf16),
                pltpu.VMEM((layers, width, ada_tiles * LANES), bf16),
                pltpu.VMEM((width, fa_tiles * LANES), bf16),
                pltpu.VMEM(w_qkv.shape[1:], bf16),
                pltpu.VMEM(w_o.shape[1:], bf16),
                pltpu.VMEM(w_up.shape[1:], bf16),
                pltpu.VMEM(w_down.shape[1:], bf16),
                pltpu.VMEM((2, layers, tokens, 2 * LANES), bf16),
                pltpu.VMEM((2, layers, head_dim, tokens), bf16),
                pltpu.VMEM((members, block_rows, 2 * LANES), bf16),
                pltpu.VMEM((half_rows, LANES), bf16),
                pltpu.VMEM((members, block_rows, LANES), bf16),
                pltpu.VMEM((ada_rows, LANES), f32),
                pltpu.VMEM((members, ada_rows, LANES), f32),
                pltpu.VMEM((2 * layers, w_ada.shape[2]), f32),
                pltpu.VMEM((2, w_fa.shape[1]), f32),
                pltpu.VMEM(b_layer.shape, bf16),
                pltpu.VMEM(b_layer.shape, f32),
                pltpu.VMEM((block_rows, width), bf16),
                pltpu.VMEM((latent_dim, block_rows), f32),
                pltpu.VMEM((block_rows, width), bf16),
                pltpu.VMEM((half_rows * (2 * head_dim - LANES) // LANES, LANES), bf16),
                pltpu.VMEM((layers, half_rows * (2 * head_dim - LANES) // LANES, LANES), bf16),
                dma((4,)), dma((8,)), dma((members,)), dma((members,)), dma((members,)), dma((members,)), dma((members,)), dma((members,)),
                dma((layers,)), dma((layers,)), dma((chips_y,)), dma((chips_y,)), dma((layers,)), dma((layers,)),
            ],
            compiler_params=pltpu.CompilerParams(collective_id=0, has_side_effects=True, vmem_limit_bytes=60 * 1024 * 1024),
        )(condition, step_size, w_in, b_fa, w_out.T, latent_t, pos_embed, b_layer, k_t, v_t, w_ada, w_fa, w_qkv, w_o, w_up, w_down)
        return jnp.transpose(result, (0, 2, 1))

    return jax.shard_map(device_fn, mesh=mesh, in_specs=in_specs, out_specs=row_spec, check_vma=False)
```

```python
import functools

import jax
import jax.numpy as jnp
from jax import lax
from jax.experimental import pallas as pl
from jax.experimental.pallas import tpu as pltpu
from jax.sharding import PartitionSpec as P

LN_EPS = 1e-6
LANES = 128
LOG2_E = 1.4426950408889634
MESH = pl.DeviceIdType.MESH


def normalize(hidden):
    mean_val = jnp.mean(hidden, axis=-1, keepdims=True)
    centered = hidden - mean_val
    var_val = jnp.mean(centered * centered, axis=-1, keepdims=True)
    return centered * lax.rsqrt(var_val + LN_EPS)


def kernel(dims, cond_ref, step_ref, w_in_ref, b_fa_ref, w_out_ref,
           latent_hbm, pos_hbm, b_layer_hbm, k_hbm, v_hbm, w_ada_hbm, w_fa_hbm, w_qkv_hbm, w_o_hbm, w_up_hbm, w_down_hbm,
           out_ref,
           head_w, ada_w, fa_w, qkv_w, o_w, up_w, down_w, kv, old_s, msg, o_msg, o_in, ada_msg, ada_in,
           mod_s, fmod_s, bias_in, bias_s, hid_s, lat_s, pos_s, pack_out, pack_in,
           w_sem, load_sem, ada_ss, ada_rs, qkv_ss, qkv_rs, o_ss, o_rs, fwd_ss, fwd_rs, out_ss, out_rs, pack_ss, pack_rs):
    (chips_x, chips_y, layers, block_rows, width, heads, head_dim) = dims
    blocks = 2 * chips_x
    patch_rows = block_rows * blocks
    half_rows = 2 * patch_rows
    members = 2 * blocks
    far_order = sorted(range(chips_x), key=lambda d: -min(d, chips_x - d))
    dp = lax.axis_index("dp")
    y = lax.axis_index("pp")
    s = lax.axis_index("sp")
    x = s // 2
    core = s % 2
    upper = y // 2
    lane_row = y % 2
    own_group = jnp.where(upper == 0, lane_row, 1 - lane_row)
    my_head = own_group * blocks + s
    row_own = pl.multiple_of(y * patch_rows + s * block_rows, block_rows)

    def group_row(group):
        return jnp.where(upper == 0, group, chips_y - 1 - group)

    def column(dx, dc):
        return 2 * ((x + dx) % chips_x) + (core + dc) % 2

    def device_row(head):
        return group_row(head // blocks)

    def dev(head):
        return (dp, device_row(head), head % blocks)

    others = [(flip, dx, dc) for flip in (1, 0) for dx in far_order for dc in (1, 0) if (flip, dx, dc) != (0, 0, 0)]

    def member(flip, dx, dc):
        return (own_group + flip) % 2 * blocks + column(dx, dc)

    partner = (dp, chips_y - 1 - y, s)

    ada_tiles = ada_w.shape[2] // LANES
    ada_total = w_ada_hbm.shape[2] // LANES
    fa_tiles = fa_w.shape[1] // LANES
    fa_total = w_fa_hbm.shape[1] // LANES

    ada_col = pl.multiple_of(jnp.minimum(ada_tiles * my_head, ada_total - ada_tiles) * LANES, LANES)
    fa_col = pl.multiple_of(jnp.minimum(fa_tiles * my_head, fa_total - fa_tiles) * LANES, LANES)
    head_copy = pltpu.make_async_copy(w_ada_hbm.at[0, :, pl.ds(0, head_w.shape[1])], head_w, load_sem.at[0])
    head_copy.start()
    bias_copy = pltpu.make_async_copy(b_layer_hbm, bias_in, load_sem.at[2])
    bias_copy.start()
    pos_copy = pltpu.make_async_copy(pos_hbm.at[y], pos_s, load_sem.at[3])
    pos_copy.start()
    lat_copy = pltpu.make_async_copy(latent_hbm.at[y], lat_s, load_sem.at[7])
    lat_copy.start()
    ada_copy = pltpu.make_async_copy(w_ada_hbm.at[:, :, pl.ds(ada_col, ada_w.shape[2])], ada_w, load_sem.at[6])
    fa_copy = pltpu.make_async_copy(w_fa_hbm.at[:, pl.ds(fa_col, fa_w.shape[1])], fa_w, load_sem.at[1])
    k_copy = pltpu.make_async_copy(k_hbm.at[:, my_head], old_s.at[0], load_sem.at[4])
    v_copy = pltpu.make_async_copy(v_hbm.at[:, my_head], old_s.at[1], load_sem.at[5])

    def w_copy(which, layer):
        src, dst = ((w_qkv_hbm, qkv_w), (w_o_hbm, o_w), (w_up_hbm, up_w), (w_down_hbm, down_w))[which]
        return pltpu.make_async_copy(src.at[layer], dst, w_sem.at[which])

    w_copy(0, 0).start()

    barrier = pltpu.get_barrier_semaphore()
    for flip, dx, dc in others:
        pl.semaphore_signal(barrier, inc=1, device_id=dev(member(flip, dx, dc)), device_id_type=MESH)
    for k in range(2):
        pl.semaphore_signal(barrier, inc=1, device_id=(dp, (1 - upper) * 2 + k, s), device_id_type=MESH)

    def activation():
        cond = cond_ref[...].astype(jnp.float32)
        return (cond * jax.nn.sigmoid(cond)).astype(jnp.bfloat16)

    def put_rows(row, value, count):
        for t in range(2):
            for i in range(count):
                at = row + t * count + i
                ada_msg[at:at + 1, :] = value[t:t + 1, i * LANES:(i + 1) * LANES]

    def ada_send(other):
        dest = member(*other)
        return pltpu.make_async_remote_copy(ada_msg, ada_in.at[my_head], ada_ss.at[dest], ada_rs.at[my_head], device_id=dev(dest), device_id_type=MESH)

    def ada_recv(other):
        src = member(*other)
        return pltpu.make_async_remote_copy(ada_msg, ada_in.at[src], ada_ss.at[src], ada_rs.at[src], device_id=dev(src), device_id_type=MESH)

    def take_rows(base, layer):
        for t in range(2):
            for tile in range(ada_total):
                part = min(tile // ada_tiles, -(-ada_total // ada_tiles) - 1)
                first = min(ada_tiles * part, ada_total - ada_tiles)
                row = base + t * ada_tiles + tile - first
                cols = slice(tile * LANES, (tile + 1) * LANES)
                mod_s[t * layers + layer:t * layers + layer + 1, cols] = ada_in[part, row:row + 1, :] + bias_s[layer:layer + 1, cols]

    bias_copy.wait()
    bias_s[...] = bias_in[...].astype(jnp.float32)
    head_copy.wait()
    ada_copy.start()
    fa_copy.start()
    k_copy.start()
    v_copy.start()
    head_res = jnp.dot(activation(), head_w[...], preferred_element_type=jnp.float32)
    for t in range(2):
        mod_s[t * layers:t * layers + 1, :2 * width] = head_res[t:t + 1] + bias_s[0:1, :2 * width]
    lat_copy.wait()
    pos_copy.wait()
    pl.semaphore_wait(barrier, members + 1)

    lane2 = lax.broadcasted_iota(jnp.int32, (1, 2 * LANES), 1)
    lane1 = lax.broadcasted_iota(jnp.int32, (1, LANES), 1)
    factor = LOG2_E * head_dim ** -0.5
    tiles = width // LANES
    group_tiles = -(-(blocks * head_dim) // LANES)
    rest = 2 * head_dim - LANES
    packs = LANES // rest
    pack_rows = half_rows // packs

    def layer_pass(it, carry):
        t = it // layers
        layer = it % layers
        following = (it + 1) % layers
        more = it + 1 < 2 * layers
        fresh = 1 - t
        bias = lambda lo, hi: bias_s[pl.ds(layer, 1), lo * width:hi * width]
        mod = lambda i: mod_s[pl.ds(it, 1), i * width:(i + 1) * width]

        @pl.when(layer == 0)
        def _():
            emb = lax.dot_general(lat_s[...].astype(jnp.bfloat16), w_in_ref[...], (((0,), (0,)), ((), ())), preferred_element_type=jnp.float32)
            hid_s[...] = (emb + pos_s[...].astype(jnp.float32)).astype(jnp.bfloat16)

        normed = (normalize(hid_s[...].astype(jnp.float32)) * (1.0 + mod(0)) + mod(1)).astype(jnp.bfloat16)
        w_copy(0, layer).wait()

        @pl.when(it == 0)
        def _():
            for which in range(1, 4):
                w_copy(which, 0).start()

        def qkv_send(dest):
            return pltpu.make_async_remote_copy(msg.at[dest], kv.at[fresh, layer, pl.ds(row_own, block_rows), :], qkv_ss.at[dest], qkv_rs.at[my_head], device_id=dev(dest), device_id_type=MESH)

        def qkv_recv(src):
            rows = pl.ds(pl.multiple_of(device_row(src) * patch_rows + src % blocks * block_rows, block_rows), block_rows)
            return pltpu.make_async_remote_copy(msg.at[src], kv.at[fresh, layer, rows, :], qkv_ss.at[src], qkv_rs.at[src], device_id=dev(src), device_id_type=MESH)

        far = 1 - own_group
        wide = group_tiles * LANES
        narrow = width - wide
        far_col = far * narrow
        near_col = (1 - far) * wide
        shift_unit = blocks * head_dim - narrow

        def columns(i, start, size):
            cols = pl.ds(pl.multiple_of(i * width + start, LANES), size)
            bias_cols = pl.ds(pl.multiple_of((6 + i) * width + start, LANES), size)
            part = jnp.dot(normed, qkv_w[:, cols], preferred_element_type=jnp.float32) + bias_s[pl.ds(layer, 1), bias_cols]
            return part.astype(jnp.bfloat16).astype(jnp.float32)

        def pack_group(group, parts):
            parts = [jnp.where(group == 1, pltpu.roll(part, wide - shift_unit, 1), part) for part in parts]

            def window(i, col, place):
                tile = min(col // LANES, group_tiles - 2)
                shift = (place - (col - tile * LANES)) % (2 * LANES)
                part = parts[i][:, tile * LANES:(tile + 2) * LANES]
                return pltpu.roll(part, shift, 1) if shift else part

            for k in range(blocks):
                col = k * head_dim
                block = jnp.where(lane2 < head_dim, window(1, col, 0),
                                  jnp.where(lane2 < 2 * head_dim, window(2, col, head_dim), window(0, col, 2 * head_dim)))
                msg[group * blocks + k] = block.astype(jnp.bfloat16)

        firsts = [columns(i, far_col, wide) for i in range(3)]
        pack_group(far, firsts)
        for dx in far_order:
            for dc in (1, 0):
                qkv_send(far * blocks + column(dx, dc)).start()
        seconds = [columns(i, near_col, narrow) for i in range(3)]
        pack_group(own_group, [jnp.where(far == 0, jnp.concatenate([first[:, narrow:], second], axis=1), jnp.concatenate([second, first[:, :wide - narrow]], axis=1))
                               for first, second in zip(firsts, seconds)])
        for dx in far_order:
            for dc in (1, 0):
                if (dx, dc) != (0, 0):
                    qkv_send(own_group * blocks + column(dx, dc)).start()
        kv[fresh, layer, pl.ds(row_own, block_rows), :] = msg[my_head]

        @pl.when(more)
        def _():
            w_copy(0, following).start()

        @pl.when(it == 0)
        def _():
            act = activation()
            ada_copy.wait()
            for part_layer in range(layers):
                put_rows(part_layer * 2 * ada_tiles, jnp.dot(act, ada_w[part_layer], preferred_element_type=jnp.float32), ada_tiles)
            fa_copy.wait()
            put_rows(layers * 2 * ada_tiles, jnp.dot(act, fa_w[...], preferred_element_type=jnp.float32), fa_tiles)
            for other in others:
                ada_send(other).start()
            ada_in[my_head] = ada_msg[...]
            k_copy.wait()
            v_copy.wait()

        @pl.when(t == 0)
        def _():
            for kp in range(1, chips_y):
                @pl.when(kp > 2 * upper)
                def _():
                    rows = slice(kp * patch_rows, (kp + 1) * patch_rows)
                    stack = jnp.concatenate([old_s[0, layer, :, rows].astype(jnp.float32), old_s[1, layer, :, rows].astype(jnp.float32),
                                             jnp.zeros((2 * LANES - 2 * head_dim, patch_rows), jnp.float32)], axis=0)
                    kv[0, layer, rows, :] = stack.T.astype(jnp.bfloat16)

        for other in others:
            qkv_recv(member(*other)).wait_recv()

        def lower_copies():
            rows = pl.ds(0, half_rows)
            return (pltpu.make_async_remote_copy(kv.at[fresh, layer, rows, pl.ds(0, LANES)], kv.at[fresh, layer, rows, pl.ds(0, LANES)], fwd_ss.at[layer], fwd_rs.at[layer], device_id=partner, device_id_type=MESH),
                    pltpu.make_async_remote_copy(pack_out, pack_in.at[layer], pack_ss.at[layer], pack_rs.at[layer], device_id=partner, device_id_type=MESH))

        def stored_copy():
            rows = pl.ds(half_rows, half_rows)
            return pltpu.make_async_remote_copy(kv.at[1, layer, rows, :], kv.at[1, layer, rows, :], fwd_ss.at[layer], fwd_rs.at[layer], device_id=partner, device_id_type=MESH)

        @pl.when(jnp.logical_and(upper == 0, t == 1))
        def _():
            stored_copy().wait_recv()

        @pl.when(upper == 0)
        def _():
            packed = None
            for r in range(packs):
                part = kv[fresh, layer, r * pack_rows:(r + 1) * pack_rows, LANES:].astype(jnp.float32)
                if r:
                    part = pltpu.roll(part, r * rest, 1)
                packed = part if packed is None else jnp.where(lane1 >= r * rest, part, packed)
            pack_out[...] = packed.astype(jnp.bfloat16)
            for copy in lower_copies():
                copy.start()

        @pl.when(upper == 1)
        def _():
            for copy in lower_copies():
                copy.wait_recv()
            packed = pack_in[layer].astype(jnp.float32)
            for r in range(packs):
                part = pltpu.roll(packed, LANES - r * rest, 1) if r else packed
                kv[fresh, layer, r * pack_rows:(r + 1) * pack_rows, LANES:] = part.astype(jnp.bfloat16)

        def o_send(p, col):
            rows = pl.ds(pl.multiple_of((p % 2) * patch_rows + col * block_rows, block_rows), block_rows)
            dest = jnp.where(p == y, own_group, 1 - own_group) * blocks + col
            return pltpu.make_async_remote_copy(o_msg.at[rows, :], o_in.at[my_head], o_ss.at[dest], o_rs.at[my_head], device_id=(dp, p, col), device_id_type=MESH)

        def o_recv(src):
            return pltpu.make_async_remote_copy(o_msg.at[pl.ds(0, block_rows), :], o_in.at[src], o_ss.at[src], o_rs.at[src], device_id=dev(src), device_id_type=MESH)

        pair = 2 * block_rows

        def queries(flip, dxs):
            p = 2 * upper + (lane_row + flip) % 2
            offsets = [(x + dx) % chips_x * pair for dx in dxs]
            if len(dxs) == chips_x:
                q_part = kv[fresh, layer, pl.ds(pl.multiple_of(p * patch_rows, patch_rows), patch_rows), LANES:]
            else:
                q_part = jnp.concatenate([kv[fresh, layer, pl.ds(pl.multiple_of(p * patch_rows + at, pair), pair), LANES:] for at in offsets], axis=0)
            q_part = pltpu.roll(q_part.astype(jnp.float32), 2 * LANES - 2 * head_dim, 1)
            return jnp.where(lane1 < head_dim, q_part, 0.0).astype(jnp.bfloat16)

        def blocks_of(flip, lanes):
            p = 2 * upper + (lane_row + flip) % 2
            return [kv[jnp.where(kp <= p, fresh, 1 - fresh), layer, kp * patch_rows:(kp + 1) * patch_rows, :lanes] for kp in range(chips_y)]

        def score(flip, dxs):
            q_part = queries(flip, dxs)
            return [lax.dot_general(q_part, block, (((1,), (1,)), ((), ())), preferred_element_type=jnp.float32) for block in blocks_of(flip, LANES)]

        def probs(scores):
            scores = jnp.concatenate(scores, axis=1)
            top = jnp.max(scores, axis=-1, keepdims=True)
            e = jnp.exp2((scores - top) * factor)
            return (e * (1.0 / jnp.sum(e, axis=-1, keepdims=True))).astype(jnp.bfloat16)

        def values(flip, dxs, prob):
            p = 2 * upper + (lane_row + flip) % 2
            o = None
            for kp, block in enumerate(blocks_of(flip, 2 * LANES)):
                term = jnp.dot(prob[:, kp * patch_rows:(kp + 1) * patch_rows], block, preferred_element_type=jnp.float32)
                o = term if o is None else o + term
            o = pltpu.roll(o, 2 * LANES - head_dim, 1)[:, :LANES].astype(jnp.bfloat16)
            if len(dxs) == chips_x:
                o_msg[pl.ds(pl.multiple_of((p % 2) * patch_rows, patch_rows), patch_rows), :] = o
            else:
                for i, dx in enumerate(dxs):
                    o_msg[pl.ds(pl.multiple_of((p % 2) * patch_rows + (x + dx) % chips_x * pair, pair), pair), :] = o[i * pair:(i + 1) * pair]

        def send_rows(flip, dxs):
            p = 2 * upper + (lane_row + flip) % 2
            for dx in dxs:
                for dc in (1, 0):
                    if (flip, dx, dc) != (0, 0, 0):
                        o_send(p, column(dx, dc)).start()

        chunks = [(flip, far_order) for flip in (1, 0)]
        all_scores = [score(*chunk) for chunk in chunks]
        all_probs = [probs(scores) for scores in all_scores]
        for (flip, dxs), prob in zip(chunks, all_probs):
            values(flip, dxs, prob)
        for flip, dxs in chunks:
            send_rows(flip, dxs)

        o_in[my_head] = o_msg[pl.ds(pl.multiple_of(lane_row * patch_rows + s * block_rows, block_rows), block_rows), :]

        @pl.when(jnp.logical_and(upper == 1, t == 0))
        def _():
            stored_copy().start()

        @pl.when(it == 0)
        def _():
            for other in others:
                ada_recv(other).wait_recv()
            for late in range(layers):
                take_rows(late * 2 * ada_tiles, late)
            for step in range(2):
                for tile in range(fa_total):
                    row = layers * 2 * ada_tiles + step * fa_tiles + tile % fa_tiles
                    cols = slice(tile * LANES, (tile + 1) * LANES)
                    fmod_s[step:step + 1, cols] = ada_in[tile // fa_tiles, row:row + 1, :] + b_fa_ref[cols].astype(jnp.float32).reshape(1, LANES)
            for other in others:
                ada_send(other).wait_send()

        for other in others:
            o_recv(member(*other)).wait_recv()

        pieces = [None] * tiles
        for head in range(heads):
            at = head * head_dim
            tile, off = at // LANES, at % LANES
            part = o_in[head].astype(jnp.float32)
            if off:
                part = pltpu.roll(part, off, 1)
            pieces[tile] = part if pieces[tile] is None else jnp.where(lane1 >= off, part, pieces[tile])
            if off + head_dim > LANES:
                pieces[tile + 1] = part
        attn = jnp.concatenate(pieces, axis=1).astype(jnp.bfloat16)
        w_copy(1, layer).wait()
        proj = jnp.dot(attn, o_w[...], preferred_element_type=jnp.float32) + bias(9, 10)

        @pl.when(more)
        def _():
            w_copy(1, following).start()

        residual = hid_s[...].astype(jnp.float32) + mod(2) * proj
        mlp_in = (normalize(residual) * (1.0 + mod(3)) + mod(4)).astype(jnp.bfloat16)
        w_copy(2, layer).wait()
        up_cols = up_w.shape[1] // 6
        w_copy(3, layer).wait()
        down = bias(14, 15)
        for i in range(6):
            cols = slice(i * up_cols, (i + 1) * up_cols)
            up_bias = bias_s[pl.ds(layer, 1), 10 * width + i * up_cols:10 * width + (i + 1) * up_cols]
            up = jnp.dot(mlp_in, up_w[:, cols], preferred_element_type=jnp.float32) + up_bias
            mid = jax.nn.gelu(up, approximate=True).astype(jnp.bfloat16)
            down = down + jnp.dot(mid, down_w[cols, :], preferred_element_type=jnp.float32)

        @pl.when(more)
        def _():
            w_copy(2, following).start()

        hid_s[...] = (residual + mod(5) * down).astype(jnp.bfloat16)

        @pl.when(more)
        def _():
            w_copy(3, following).start()

        @pl.when(layer == layers - 1)
        def _():
            scale_out = fmod_s[pl.ds(t, 1), :width]
            shift_out = fmod_s[pl.ds(t, 1), width:]
            out_rows = (normalize(hid_s[...].astype(jnp.float32)) * (1.0 + scale_out) + shift_out).astype(jnp.bfloat16)
            velocity = lax.dot_general(w_out_ref[...], out_rows, (((1,), (1,)), ((), ())), preferred_element_type=jnp.float32)
            lat_s[...] = lat_s[...] + step_ref[t] * velocity

        for other in others:
            qkv_send(member(*other)).wait_send()
            flip, dx, dc = other
            o_send(2 * upper + (lane_row + flip) % 2, column(dx, dc)).wait_send()

        @pl.when(upper == 0)
        def _():
            for copy in lower_copies():
                copy.wait_send()

        @pl.when(jnp.logical_and(upper == 1, t == 0))
        def _():
            stored_copy().wait_send()

        return carry

    lax.fori_loop(0, 2 * layers, layer_pass, 0)

    def out_copy(k, src_side):
        row = (y + k) % chips_y
        slot = row if src_side else y
        return pltpu.make_async_remote_copy(lat_s, out_ref.at[slot], out_ss.at[row], out_rs.at[slot], device_id=(dp, row, s), device_id_type=MESH)

    for k in range(1, chips_y):
        out_copy(k, False).start()
    own_copy = pltpu.make_async_copy(lat_s, out_ref.at[y], load_sem.at[0])
    own_copy.start()
    for k in range(1, chips_y):
        out_copy(k, True).wait_recv()
    own_copy.wait()
    for k in range(1, chips_y):
        out_copy(k, False).wait_send()


def solution(mesh):
    chips_y = mesh.shape["pp"]
    chips_x = mesh.shape["sp"] // 2
    row_spec = P("dp", "sp", None)
    full_spec = P()
    buf_spec = P("dp", None, None, None)
    in_specs = (row_spec, P(None, "sp", None), P("dp", None), P("dp"), full_spec, full_spec, full_spec, full_spec, full_spec, full_spec, full_spec, full_spec, full_spec, full_spec, buf_spec, buf_spec)

    def device_fn(latent_in, pos_embed, condition, step_size, w_in, w_ada, w_qkv, w_o, w_up, w_down, b_layer, w_fa, b_fa, w_out, k_old, v_old):
        patches, block_rows, latent_dim = latent_in.shape
        layers, width = w_qkv.shape[:2]
        tokens, heads, head_dim = k_old.shape[1:]
        members = 4 * chips_x
        ada_tiles = -(-(w_ada.shape[2] // LANES) // members)
        fa_tiles = -(-(w_fa.shape[1] // LANES) // members)
        ada_rows = 2 * (layers * ada_tiles + fa_tiles)
        half_rows = 2 * block_rows * 2 * chips_x
        dims = (chips_x, chips_y, layers, block_rows, width, heads, head_dim)
        bf16, f32 = jnp.bfloat16, jnp.float32
        vmem = pl.BlockSpec(memory_space=pltpu.VMEM)
        hbm = pl.BlockSpec(memory_space=pl.ANY)
        dma = pltpu.SemaphoreType.DMA
        latent_t = jnp.transpose(latent_in, (0, 2, 1))
        k_t = jnp.transpose(k_old, (0, 2, 3, 1))
        v_t = jnp.transpose(v_old, (0, 2, 3, 1))
        result = pl.pallas_call(
            functools.partial(kernel, dims),
            out_shape=jax.ShapeDtypeStruct(latent_t.shape, f32),
            in_specs=[vmem, pl.BlockSpec(memory_space=pltpu.SMEM), vmem, vmem, vmem] + [hbm] * 11,
            out_specs=hbm,
            scratch_shapes=[
                pltpu.VMEM((width, 2 * width), bf16),
                pltpu.VMEM((layers, width, ada_tiles * LANES), bf16),
                pltpu.VMEM((width, fa_tiles * LANES), bf16),
                pltpu.VMEM(w_qkv.shape[1:], bf16),
                pltpu.VMEM(w_o.shape[1:], bf16),
                pltpu.VMEM(w_up.shape[1:], bf16),
                pltpu.VMEM(w_down.shape[1:], bf16),
                pltpu.VMEM((2, layers, tokens, 2 * LANES), bf16),
                pltpu.VMEM((2, layers, head_dim, tokens), bf16),
                pltpu.VMEM((members, block_rows, 2 * LANES), bf16),
                pltpu.VMEM((half_rows, LANES), bf16),
                pltpu.VMEM((members, block_rows, LANES), bf16),
                pltpu.VMEM((ada_rows, LANES), f32),
                pltpu.VMEM((members, ada_rows, LANES), f32),
                pltpu.VMEM((2 * layers, w_ada.shape[2]), f32),
                pltpu.VMEM((2, w_fa.shape[1]), f32),
                pltpu.VMEM(b_layer.shape, bf16),
                pltpu.VMEM(b_layer.shape, f32),
                pltpu.VMEM((block_rows, width), bf16),
                pltpu.VMEM((latent_dim, block_rows), f32),
                pltpu.VMEM((block_rows, width), bf16),
                pltpu.VMEM((half_rows * (2 * head_dim - LANES) // LANES, LANES), bf16),
                pltpu.VMEM((layers, half_rows * (2 * head_dim - LANES) // LANES, LANES), bf16),
                dma((4,)), dma((8,)), dma((members,)), dma((members,)), dma((members,)), dma((members,)), dma((members,)), dma((members,)),
                dma((layers,)), dma((layers,)), dma((chips_y,)), dma((chips_y,)), dma((layers,)), dma((layers,)),
            ],
            compiler_params=pltpu.CompilerParams(collective_id=0, has_side_effects=True, vmem_limit_bytes=60 * 1024 * 1024),
        )(condition, step_size, w_in, b_fa, w_out.T, latent_t, pos_embed, b_layer, k_t, v_t, w_ada, w_fa, w_qkv, w_o, w_up, w_down)
        return jnp.transpose(result, (0, 2, 1))

    return jax.shard_map(device_fn, mesh=mesh, in_specs=in_specs, out_specs=row_spec, check_vma=False)
```
